256 devices in a mesh: rep: 2 (over y), seq: 128 (over x, z, core).
Axes of the slice: x: 4, y: 2, z: 16, core: 2. Of those that a mesh axis runs over, the one named last changes fastest.
The devices are a block of a 4x16x16 slice.
Arguments:
- tokens: bfloat16 [131072, 768], P(('rep', 'seq')), parts along dimension 0, may hold values from -60 to 60
- w_qkv: bfloat16 [768, 2304], replicated, may hold values from -0.21875 to 0.21875
- w_gate: bfloat16 [768, 36], replicated, may hold values from -0.21875 to 0.21875
- w_out: bfloat16 [768, 768], replicated, may hold values from -0.21875 to 0.21875
- cmp_med: bfloat16 [2, 12, 16], replicated, may hold values from -1.5 to 1.5
- cmp_coarse: bfloat16 [2, 12, 256], replicated, may hold values from -0.375 to 0.375
- group_id: int32 [8192], P('rep'), parts along dimension 0, may hold values from 0 to 63, never falling along the last dimension, each value on 1 to 96 neighbouring positions
Outputs:
- layer_out: bfloat16 [131072, 768], P(('rep', 'seq')), parts along dimension 0
The draws below stay inside these ranges and needn't reach their ends.
There are 2 independent parts, one for each index of `rep`. The reference program is written for one: setup_inputs(seed, part) draws one part's arguments, and reference() takes and returns one part's arrays. A program takes and returns all parts, laid end to end along the dimension named above; an argument that names none is the same for every part. Nothing has to cross between parts.
Inputs may be any that keep to these rules, and one draw needn't show every extreme that they name: `group_id`: never falling along the blocks; each sub-group holds 1 to 96 consecutive blocks, and one holds exactly that many.
All inputs are finite; a program needn't handle non-finite values.
Results may differ from the reference program's by a relative error of at most 0.012.
The reference program's roundings to bfloat16 on the way count: a program that leaves them out, or rounds other values in their place, can miss the bound.
Values may be sent and summed in bfloat16 or wider, within the bound.
No kernel may reach another device: no remote copies, remote signals or barrier semaphores. Data moves between devices by JAX's collectives and lax.ppermute only.
A program may use at most 128 MiB of HBM per device.

```python
import math
import jax
import jax.numpy as jnp
import numpy as np
from jax import lax

D = 768
HEADS = 12
HEAD_DIM = 64
TOK_DEV = 512
WINDOW = 128
MED = 16
COARSE = 256
REACH = 3
INNER = 768
TOKENS = 65536
NBLK = 4096
N_SEQ = 128


def draw_tokens(key, part):
    values_drawn = jax.random.truncated_normal(key, -6.0, 6.0, (TOKENS, D), jnp.float32)
    return values_drawn.astype(jnp.bfloat16)


def split_up(number_of, total, reach, lean):
    portions = [(1 << 20) // math.isqrt(rank ** lean) + 1 for rank in range(2, number_of + 1)]
    rest, counts = total - reach - (number_of - 1), [1] * (number_of - 1)
    while rest > 0:
        candidates = [i for i in range(number_of - 1) if counts[i] < reach]
        pool, remaining = sum([portions[i] for i in candidates]), rest
        for i in candidates:
            more = min(reach - counts[i], max(1, remaining * portions[i] // pool), rest)
            counts[i] = counts[i] + more
            rest = rest - more
    return np.array([reach] + counts)


def ragged(stream_key, amount, total, limit, slope):
    if amount == 2:
        one = jax.random.randint(stream_key, (), max(1, total - limit), min(limit, total - 1) + 1)
        return jnp.stack([one, total - one])
    lengths = jnp.asarray(split_up(amount, total, limit, slope), jnp.int32)
    couples = (amount - 1) // 2
    giver, receiver = lengths[1:1 + 2 * couples:2], lengths[2:2 + 2 * couples:2]
    room = jnp.minimum(giver - 1, limit - receiver)
    moved = jax.random.randint(jax.random.fold_in(stream_key, 1), (couples,), 0, 1 << 20) % (room + 1)
    lengths = lengths.at[1:1 + 2 * couples:2].set(giver - moved).at[2:2 + 2 * couples:2].set(receiver + moved)
    return lengths[jax.random.permutation(jax.random.fold_in(stream_key, 2), amount)]


def normal_values(own_key, extent, scale, bound, held_as=jnp.bfloat16):
    return jnp.clip(scale * jax.random.normal(own_key, extent, jnp.float32), -bound, bound).astype(held_as)


def setup_inputs(seed: int = 0, part: int = 0) -> dict:
    streams_of = jax.random.split(jax.random.key(seed), 8)
    own_keys = jax.random.split(jax.random.fold_in(streams_of[7], part), 8)
    tokens = draw_tokens(jax.random.fold_in(jax.random.fold_in(streams_of[7], part), 71), part)
    w_qkv = normal_values(streams_of[1], (D, 3 * INNER), D ** -0.5, 0.21875)
    w_gate = normal_values(streams_of[2], (D, 3 * HEADS), D ** -0.5, 0.21875)
    w_out = normal_values(streams_of[3], (INNER, D), INNER ** -0.5, 0.21875)
    cmp_med = normal_values(streams_of[4], (2, HEADS, MED), MED ** -0.5, 1.5)
    cmp_coarse = normal_values(streams_of[5], (2, HEADS, COARSE), COARSE ** -0.5, 0.375)
    group_id = jnp.searchsorted(jnp.cumsum(ragged(own_keys[6], N_SEQ // 2, NBLK, REACH * TOK_DEV // MED, 1)), jnp.arange(NBLK), side="right").astype(jnp.int32)
    return {"tokens": tokens, "w_qkv": w_qkv, "w_gate": w_gate, "w_out": w_out, "cmp_med": cmp_med, "cmp_coarse": cmp_coarse, "group_id": group_id}


def compress(row_data, weights, block_len):
    blocks = row_data.shape[0] // block_len
    shaped = row_data.reshape(blocks, block_len, HEADS, HEAD_DIM).astype(jnp.float32)
    packed = jnp.einsum('bjhd,hj->bhd', shaped, weights.astype(jnp.float32), precision=lax.Precision.HIGHEST)
    return packed.reshape(blocks, HEADS * HEAD_DIM).astype(jnp.bfloat16)


def sink_attend(scores, visible, value_rows):
    masked = jnp.where(visible[:, None, :], scores, -1e30)
    row_peak = jnp.maximum(jnp.max(masked, axis=-1, keepdims=True), 0.0)
    exp_terms = jnp.where(visible[:, None, :], jnp.exp(masked - row_peak), 0.0)
    denominator = jnp.exp(-row_peak) + jnp.sum(exp_terms, axis=-1, keepdims=True)
    weights = (exp_terms / denominator).astype(jnp.bfloat16)
    return jnp.einsum('qhk,khd->qhd', weights.astype(jnp.float32), value_rows.astype(jnp.float32), precision=lax.Precision.HIGHEST)


def reference(tokens, w_qkv, w_gate, w_out, cmp_med, cmp_coarse, group_id):
    inner = HEADS * HEAD_DIM
    scale = HEAD_DIM ** -0.5
    block_rows = min(512, TOK_DEV)
    projected = jnp.dot(tokens, w_qkv, preferred_element_type=jnp.float32).astype(jnp.bfloat16)
    queries = projected[:, :inner]
    key_rows = projected[:, inner:2 * inner]
    value_rows = projected[:, 2 * inner:]
    gate_values = jax.nn.sigmoid(jnp.dot(tokens, w_gate, preferred_element_type=jnp.float32))
    med_keys = compress(key_rows, cmp_med[0], MED)
    med_values = compress(value_rows, cmp_med[1], MED)
    coarse_keys = compress(key_rows, cmp_coarse[0], COARSE).reshape(-1, HEADS, HEAD_DIM)
    coarse_values = compress(value_rows, cmp_coarse[1], COARSE).reshape(-1, HEADS, HEAD_DIM)
    coarse_count = TOKENS // COARSE
    coarse_index = jnp.arange(coarse_count, dtype=jnp.int32)
    padded_keys = jnp.concatenate([jnp.zeros((WINDOW, inner), jnp.bfloat16), key_rows], 0)
    padded_values = jnp.concatenate([jnp.zeros((WINDOW, inner), jnp.bfloat16), value_rows], 0)
    most_blocks = REACH * TOK_DEV // MED
    key_span = most_blocks + block_rows // MED
    total_blocks = TOKENS // MED
    token_groups = jnp.repeat(group_id, MED)

    def one_block(block_index):
        row_start = block_index * block_rows
        query_block = lax.dynamic_slice_in_dim(queries, row_start, block_rows, 0).reshape(block_rows, HEADS, HEAD_DIM).astype(jnp.float32)
        positions = row_start + jnp.arange(block_rows, dtype=jnp.int32)
        win_keys = lax.dynamic_slice_in_dim(padded_keys, row_start, block_rows + WINDOW, 0).reshape(-1, HEADS, HEAD_DIM)
        win_values = lax.dynamic_slice_in_dim(padded_values, row_start, block_rows + WINDOW, 0).reshape(-1, HEADS, HEAD_DIM)
        key_pos = row_start - WINDOW + jnp.arange(block_rows + WINDOW, dtype=jnp.int32)
        visible = (key_pos[None, :] <= positions[:, None]) & (key_pos[None, :] > positions[:, None] - WINDOW) & (key_pos[None, :] >= 0)
        scores = jnp.einsum('qhd,khd->qhk', query_block, win_keys.astype(jnp.float32), precision=lax.Precision.HIGHEST) * scale
        masked = jnp.where(visible[:, None, :], scores, -1e30)
        row_peak = jnp.max(masked, axis=-1, keepdims=True)
        exp_terms = jnp.where(visible[:, None, :], jnp.exp(masked - row_peak), 0.0)
        weights_low = (exp_terms / jnp.sum(exp_terms, axis=-1, keepdims=True)).astype(jnp.bfloat16)
        window_out = jnp.einsum('qhk,khd->qhd', weights_low.astype(jnp.float32), win_values.astype(jnp.float32), precision=lax.Precision.HIGHEST)
        block_first = jnp.clip(row_start // MED - most_blocks, 0, total_blocks - key_span).astype(jnp.int32)
        near_keys = lax.dynamic_slice_in_dim(med_keys, block_first, key_span, 0).reshape(key_span, HEADS, HEAD_DIM)
        near_values = lax.dynamic_slice_in_dim(med_values, block_first, key_span, 0).reshape(key_span, HEADS, HEAD_DIM)
        key_groups = lax.dynamic_slice_in_dim(group_id, block_first, key_span, 0)
        key_blocks = block_first + jnp.arange(key_span, dtype=jnp.int32)
        query_groups = lax.dynamic_slice_in_dim(token_groups, row_start, block_rows, 0)
        visible_med = (key_groups[None, :] == query_groups[:, None]) & (key_blocks[None, :] * MED + MED - 1 <= positions[:, None])
        med_scores = jnp.einsum('qhd,khd->qhk', query_block, near_keys.astype(jnp.float32), precision=lax.Precision.HIGHEST) * scale
        medium_out = sink_attend(med_scores, visible_med, near_values)
        visible_coarse = coarse_index[None, :] * COARSE + COARSE - 1 <= positions[:, None]
        coarse_scores = jnp.einsum('qhd,khd->qhk', query_block, coarse_keys.astype(jnp.float32), precision=lax.Precision.HIGHEST) * scale
        coarse_out = sink_attend(coarse_scores, visible_coarse, coarse_values)
        gate_block = lax.dynamic_slice_in_dim(gate_values, row_start, block_rows, 0)
        mixed_heads = gate_block[:, :HEADS, None] * window_out + gate_block[:, HEADS:2 * HEADS, None] * medium_out + gate_block[:, 2 * HEADS:, None] * coarse_out
        return mixed_heads.reshape(block_rows, inner).astype(jnp.bfloat16)

    mixed_rows = lax.map(one_block, jnp.arange(TOKENS // block_rows, dtype=jnp.int32)).reshape(TOKENS, inner)
    return jnp.dot(mixed_rows, w_out, preferred_element_type=jnp.float32).astype(jnp.bfloat16)
```

```python
import jax
import jax.numpy as jnp
from jax import lax
from jax.experimental import pallas as pl
from jax.experimental.pallas import tpu as pltpu
from jax.sharding import Mesh
from jax.sharding import PartitionSpec as P

WINDOW = 128
REACH = 3
AX_X, AX_Z, AX_C = "seq_0", "seq_1", "seq_2"
SEQ = (AX_X, AX_Z, AX_C)
REP_SEQ = ("rep", AX_X, AX_Z, AX_C)
LANES = 128
NEG = -1e30
F32, BF16, I32 = jnp.float32, jnp.bfloat16, jnp.int32
NT = (((1,), (1,)), ((), ()))
TN = (((0,), (0,)), ((), ()))


def dot(a, b):
    return jnp.dot(a, b, preferred_element_type=F32)


def dot_nt(a, b):
    return lax.dot_general(a, b, NT, preferred_element_type=F32)


def iota(shape, dim):
    return lax.broadcasted_iota(I32, shape, dim)


def one_hot(condition):
    return jnp.where(condition, 1.0, 0.0).astype(BF16)


def half_lanes(rows):
    return iota((rows, LANES), 1) < LANES // 2


def token_classes(tok_rows, med_len):
    row, lane = iota((tok_rows, LANES), 0), iota((tok_rows, LANES), 1)
    wanted = 2 * (row // med_len) + jnp.where(row % med_len == med_len - 1, 1, 0)
    return one_hot(lane % (LANES // 2) == wanted)


def project_kernel(tok_ref, w_ref, cm_ref, cc_ref, kv_ref, med_ref, pay_ref, w_buf, c_buf, sems):
    tok_rows = tok_ref.shape[0]
    heads, _, med_len = cm_ref.shape
    coarse_len = cc_ref.shape[2]
    inner = kv_ref.shape[1] // 2
    width = w_buf.shape[2]
    steps = w_buf.shape[0]
    copies = []
    for g in range(steps):
        columns = pl.ds(inner + g * width, width)
        copies.append(pltpu.make_async_copy(w_ref.at[:, columns], w_buf.at[g], sems.at[g]))
        copies[-1].start()
    med_blocks = tok_rows // med_len
    coarse_blocks = tok_rows // coarse_len
    per = width // 64
    tile_up = one_hot(iota((med_len, tok_rows), 1) % med_len == iota((med_len, tok_rows), 0))
    own_block = iota((per * med_blocks, tok_rows), 0) % med_blocks == (
        iota((per * med_blocks, tok_rows), 1) // med_len
    )
    own_coarse = iota((8, tok_rows), 0) == iota((8, tok_rows), 1) // coarse_len
    mixes = []
    for g in range(steps):
        side, first = (2 * g) // steps, (g % (steps // 2)) * per
        med_rows, coarse_rows = [], []
        for i in range(per):
            med_w = cm_ref[first + i].astype(F32)[side : side + 1, :]
            med_rows.append(jnp.broadcast_to(med_w, (med_blocks, med_len)))
            coarse_w = cc_ref[first + i].astype(F32)[side : side + 1, :]
            coarse_w = jnp.concatenate([coarse_w] * coarse_blocks, axis=1)
            coarse_rows.append(jnp.where(own_coarse, jnp.broadcast_to(coarse_w, (8, tok_rows)), 0.0))
        med_mix = dot(jnp.concatenate(med_rows, 0).astype(BF16), tile_up)
        med_mix = jnp.where(own_block, med_mix, 0.0)
        mixes.append(jnp.concatenate([med_mix] + coarse_rows, 0).astype(BF16))
    for g in range(steps):
        copies[g].wait()
        rows = dot(tok_ref[...], w_buf[g]).astype(BF16)
        kv_ref[:, g * width : (g + 1) * width] = rows
        packed = dot(mixes[g], rows)
        med_head = iota((med_blocks, width), 1) // 64
        coarse_head = iota((8, width), 1) // 64
        med = jnp.zeros((med_blocks, width), F32)
        coarse = jnp.zeros((8, width), F32)
        for i in range(per):
            med = jnp.where(med_head == i, packed[i * med_blocks : (i + 1) * med_blocks], med)
            at = per * med_blocks + 8 * i
            coarse = jnp.where(coarse_head == i, packed[at : at + 8], coarse)
        med_ref[:, g * width : (g + 1) * width] = med.astype(BF16)
        for i in range(width // LANES):
            tile = g * (width // LANES) + i
            c_buf[tile * coarse_blocks : (tile + 1) * coarse_blocks, :] = coarse[
                :coarse_blocks, i * LANES : (i + 1) * LANES
            ]
    count = c_buf.shape[0]
    total = pay_ref.shape[0]
    repeat = one_hot(iota((total, count), 0) % count == iota((total, count), 1))
    pay_ref[...] = dot(repeat, c_buf[...].astype(BF16)).astype(BF16)


def values_up(tile, odd):
    eye = one_hot(iota((LANES, LANES), 0) == iota((LANES, LANES), 1))
    turned = dot_nt(eye, tile).astype(BF16)
    half = LANES // 2
    ones = jnp.ones((16, tile.shape[0]), BF16)
    return jnp.concatenate([turned[half * odd : half * (odd + 1)], ones], 0)


def near_kernel(
    tok_ref, tail_ref, w_ref, wg_ref, kv_ref, far3_ref, far2_ref, far1_ref, med_ref, gid_ref,
    q_ref, gate_ref, mix_ref, w_buf, tail_buf, bias_buf, hot_buf, sems,
):
    tok_rows, depth = tok_ref.shape
    inner = kv_ref.shape[1] // 2
    width = w_buf.shape[2]
    steps = w_buf.shape[0]
    heads = gate_ref.shape[0] // 3
    med_blocks = med_ref.shape[0]
    med_len = tok_rows // med_blocks
    near = (REACH + 1) * med_blocks
    half = LANES // 2
    copies = []
    for g in range(steps):
        copies.append(
            pltpu.make_async_copy(w_ref.at[:, pl.ds(g * width, width)], w_buf.at[g], sems.at[g])
        )
        copies[-1].start()
    position = (lax.axis_index(AX_X) * lax.axis_size(AX_Z) + lax.axis_index(AX_Z)) * lax.axis_size(
        AX_C
    ) + lax.axis_index(AX_C)
    gate_ref[...] = 1.0 / (1.0 + jnp.exp(-dot_nt(wg_ref[...], tok_ref[...])))
    hot_buf[...] = token_classes(tok_rows, med_len)

    first = (position - REACH) * med_blocks
    padded = first + near
    row = padded // LANES - 1
    offset = padded % LANES
    low = gid_ref[pl.ds(jnp.maximum(row, 0), 1), :]
    high = gid_ref[pl.ds(jnp.minimum(row + 1, gid_ref.shape[0] - 1), 1), :]
    lane = iota((1, LANES), 1)
    both = jnp.where(lane >= offset, low, high)
    near_groups = pltpu.roll(jnp.broadcast_to(both, (8, LANES)), (LANES - offset) % LANES, 1)[:1]
    near_groups = jnp.where(lane + first >= 0, near_groups, -1).astype(F32).astype(BF16)
    spread = jnp.broadcast_to(near_groups.astype(F32), (near, LANES)).astype(BF16)
    i0, i1 = iota((near, LANES), 0), iota((near, LANES), 1)
    key_group = dot_nt(one_hot(i0 == i1), spread)
    own = (i1 % half) // 2 + REACH * med_blocks
    pick = one_hot(i0 == own)
    token_group = dot(spread, pick)
    visible = (key_group == token_group) & ((i0 < own) | ((i0 == own) & (i1 % 2 == 1)))
    bias_buf[...] = jnp.where(visible, 0.0, NEG).astype(BF16)

    for g in range(steps):
        copies[g].wait()
        lo = g * width
        if lo < inner:
            rows = dot(tok_ref[...], w_buf[g]).astype(BF16).astype(F32)
            q_ref[:, lo : lo + width] = (rows * (half**-0.5)).astype(BF16)
        else:
            tail_buf[:, lo - inner : lo - inner + width] = dot(tail_ref[...], w_buf[g]).astype(BF16)

    below = iota((WINDOW, WINDOW), 0) <= iota((WINDOW, WINDOW), 1)
    chunks = tok_rows // WINDOW
    first_bias = jnp.where(position == 0, NEG, 0.0)

    @pl.loop(0, heads // 2)
    def _(pair):
        at = pl.multiple_of(pair * LANES, LANES)
        at_v = pl.multiple_of(inner + pair * LANES, LANES)
        q_tile = q_ref[:, pl.ds(at, LANES)]
        keys = jnp.concatenate([tail_buf[:, pl.ds(at, LANES)], kv_ref[:, pl.ds(at, LANES)]], 0)
        values = jnp.concatenate([tail_buf[:, pl.ds(at_v, LANES)], kv_ref[:, pl.ds(at_v, LANES)]], 0)
        blocks = (far3_ref, far2_ref, far1_ref, med_ref)
        med_k = jnp.concatenate([b[:, pl.ds(at, LANES)] for b in blocks], 0)
        med_v = jnp.concatenate([b[:, pl.ds(at_v, LANES)] for b in blocks], 0)
        for odd in range(2):
            head = 2 * pair + odd
            mine = half_lanes(tok_rows) if odd == 0 else ~half_lanes(tok_rows)
            q_ext = jnp.where(mine, q_tile, hot_buf[...])
            mine_k = half_lanes(keys.shape[0]) if odd == 0 else ~half_lanes(keys.shape[0])
            k_ext = jnp.where(mine_k, keys, jnp.zeros_like(keys))
            merged = []
            for c in range(chunks):
                s = dot_nt(
                    k_ext[c * WINDOW : (c + 2) * WINDOW], q_ext[c * WINDOW : (c + 1) * WINDOW]
                )
                left, right = s[:WINDOW], s[WINDOW:]
                if c == 0:
                    left = left + first_bias
                merged.append(jnp.where(below, right, left))
            scores = jnp.concatenate(merged, 1)
            peak = jnp.max(scores, axis=0, keepdims=True)
            terms = jnp.exp(scores - peak).astype(BF16)
            v_up = values_up(values, odd)
            outs = []
            for c in range(chunks):
                part = terms[:, c * WINDOW : (c + 1) * WINDOW]
                zero = jnp.zeros_like(part)
                both_parts = jnp.concatenate(
                    [jnp.where(below, zero, part), jnp.where(below, part, zero)], 0
                )
                outs.append(dot(v_up[:, c * WINDOW : (c + 2) * WINDOW], both_parts))
            out = jnp.concatenate(outs, 1)
            factor = gate_ref[pl.ds(head, 1), :] / out[half : half + 1]
            mixed = out[:half] * factor

            mine_m = half_lanes(near) if odd == 0 else ~half_lanes(near)
            scores = dot_nt(jnp.where(mine_m, med_k, bias_buf[...]), q_ext)
            peak = jnp.maximum(jnp.max(scores, axis=0, keepdims=True), 0.0)
            terms = jnp.exp(scores - peak).astype(BF16)
            out = dot(values_up(med_v, odd), terms)
            factor = gate_ref[pl.ds(heads + head, 1), :] / (jnp.exp(-peak) + out[half : half + 1])
            mixed = mixed + out[:half] * factor
            mix_ref[pl.ds(pl.multiple_of(head * half, half), half), :] = mixed


def far_kernel(
    q_ref, gate_ref, mix_ref, w_ref, *refs
):
    pieces, (out_ref, keys_buf, values_buf, bias_buf, hot_buf, mixed_buf) = refs[:-6], refs[-6:]
    tok_rows, inner = q_ref.shape
    heads = gate_ref.shape[0] // 3
    half = LANES // 2
    tiles = inner // LANES
    total = pieces[0].shape[0]
    zs = lax.axis_size(AX_Z)
    count = total // zs
    each = total // (2 * tiles)
    per = each // zs
    pos_x, pos_z, pos_c = lax.axis_index(AX_X), lax.axis_index(AX_Z), lax.axis_index(AX_C)
    xs, cs = lax.axis_size(AX_X), lax.axis_size(AX_C)
    hot_buf[...] = token_classes(tok_rows, 16)

    r0, r1 = iota((total, total), 0), iota((total, total), 1)
    source = ((r0 % each) // per) * count + (r0 // each) * per + r0 % per
    turn = one_hot(source == r1)
    sorted_rows = dot(turn, jnp.concatenate([p[...] for p in pieces], 1)).astype(BF16)
    lane = iota((each, LANES), 1) % half
    row = iota((each, LANES), 0)
    position = (pos_x * zs + pos_z) * cs + pos_c
    seen = per * position + jnp.where(lane >= half // per - 1, 1, 0) + jnp.where(lane == half - 1, 1, 0)
    for n in range(len(pieces)):
        for t in range(tiles):
            block = sorted_rows[t * each : (t + 1) * each, n * LANES : (n + 1) * LANES]
            keys_buf[n * each : (n + 1) * each, t * LANES : (t + 1) * LANES] = block
            block = sorted_rows[(tiles + t) * each : (tiles + t + 1) * each, n * LANES : (n + 1) * LANES]
            values_buf[n * each : (n + 1) * each, t * LANES : (t + 1) * LANES] = block
        from_x = lax.rem(pos_x + xs - n % xs, xs)
        from_c = lax.rem(pos_c + n // xs, cs)
        index = ((from_x * zs + row // per) * cs + from_c) * per + row % per
        bias_buf[n * each : (n + 1) * each, :] = jnp.where(index < seen, 0.0, NEG).astype(BF16)

    keys_count = keys_buf.shape[0]

    @pl.loop(0, tiles)
    def _(pair):
        at = pl.multiple_of(pair * LANES, LANES)
        q_tile = q_ref[:, pl.ds(at, LANES)]
        keys = keys_buf[:, pl.ds(at, LANES)]
        values = values_buf[:, pl.ds(at, LANES)]
        for odd in range(2):
            head = 2 * pair + odd
            mine = half_lanes(tok_rows) if odd == 0 else ~half_lanes(tok_rows)
            q_ext = jnp.where(mine, q_tile, hot_buf[...])
            mine_k = half_lanes(keys_count) if odd == 0 else ~half_lanes(keys_count)
            scores = dot_nt(jnp.where(mine_k, keys, bias_buf[...]), q_ext)
            peak = jnp.maximum(jnp.max(scores, axis=0, keepdims=True), 0.0)
            terms = jnp.exp(scores - peak).astype(BF16)
            out = dot(values_up(values, odd), terms)
            factor = gate_ref[pl.ds(2 * heads + head, 1), :] / (jnp.exp(-peak) + out[half : half + 1])
            rows = pl.ds(pl.multiple_of(head * half, half), half)
            mixed_buf[rows, :] = (mix_ref[rows, :] + out[:half] * factor).astype(BF16)

    out_ref[...] = lax.dot_general(
        mixed_buf[...], w_ref[...], TN, preferred_element_type=F32
    ).astype(BF16)


def shifted(block, axis, distance):
    size = lax.axis_size(axis)
    return lax.ppermute(block, axis, [(i - distance, i) for i in range(distance, size)])


def turned(block, axis, distance):
    size = lax.axis_size(axis)
    return lax.ppermute(block, axis, [(i, (i + distance) % size) for i in range(size)])


VMEM = pl.BlockSpec(memory_space=pltpu.VMEM)
HBM = pl.BlockSpec(memory_space=pl.ANY)


def params(mib):
    return pltpu.CompilerParams(vmem_limit_bytes=mib << 20)


def shards(tokens, w_qkv, w_gate, w_out, cmp_med, cmp_coarse, group_id):
    tok_rows, depth = tokens.shape
    heads, med_len, coarse_len = cmp_med.shape[1], cmp_med.shape[2], cmp_coarse.shape[2]
    inner = w_out.shape[0]
    width = 256
    med_blocks = tok_rows // med_len
    coarse_blocks = tok_rows // coarse_len
    zs = lax.axis_size(AX_Z)
    count = coarse_blocks * 2 * inner // LANES
    tail = shifted(tokens[tok_rows - WINDOW :], SEQ, 1)

    kv_steps = 2 * inner // width
    kv, med, payload = pl.pallas_call(
        project_kernel,
        out_shape=(
            jax.ShapeDtypeStruct((tok_rows, 2 * inner), BF16),
            jax.ShapeDtypeStruct((med_blocks, 2 * inner), BF16),
            jax.ShapeDtypeStruct((zs * count, LANES), BF16),
        ),
        in_specs=[VMEM, HBM, VMEM, VMEM],
        out_specs=(VMEM, VMEM, VMEM),
        scratch_shapes=[
            pltpu.VMEM((kv_steps, depth, width), BF16),
            pltpu.VMEM((count, LANES), F32),
            pltpu.SemaphoreType.DMA((kv_steps,)),
        ],
        compiler_params=params(24),
        cost_estimate=pl.CostEstimate(flops=2 * tok_rows * depth * 2 * inner, bytes_accessed=4 << 20, transcendentals=0),
        name="project",
    )(tokens, w_qkv, cmp_med.transpose(1, 0, 2), cmp_coarse.transpose(1, 0, 2))

    column = lax.all_to_all(payload, AX_Z, 0, 0, tiled=True)
    far1, far2, far3 = (shifted(med, SEQ, k) for k in (1, 2, 3))

    all_steps = 3 * inner // width
    q, gates, mixed = pl.pallas_call(
        near_kernel,
        out_shape=(
            jax.ShapeDtypeStruct((tok_rows, inner), BF16),
            jax.ShapeDtypeStruct((3 * heads, tok_rows), F32),
            jax.ShapeDtypeStruct((inner, tok_rows), F32),
        ),
        in_specs=[VMEM, VMEM, HBM] + [VMEM] * 7,
        out_specs=(VMEM, VMEM, VMEM),
        scratch_shapes=[
            pltpu.VMEM((all_steps, depth, width), BF16),
            pltpu.VMEM((WINDOW, 2 * inner), BF16),
            pltpu.VMEM(((REACH + 1) * med_blocks, LANES), BF16),
            pltpu.VMEM((tok_rows, LANES), BF16),
            pltpu.SemaphoreType.DMA((all_steps,)),
        ],
        compiler_params=params(30),
        cost_estimate=pl.CostEstimate(flops=4 << 30, bytes_accessed=8 << 20, transcendentals=0),
        name="near",
    )(tokens, tail, w_qkv, w_gate.T, kv, far3, far2, far1, med, group_id.reshape(-1, LANES))

    columns = [column] + [turned(column, AX_X, k) for k in range(1, lax.axis_size(AX_X))]
    columns += [turned(c, AX_C, 1) for c in columns]
    keys_count = coarse_blocks * lax.axis_size(SEQ)
    return pl.pallas_call(
        far_kernel,
        out_shape=jax.ShapeDtypeStruct((tok_rows, inner), BF16),
        in_specs=[VMEM] * (4 + len(columns)),
        out_specs=VMEM,
        scratch_shapes=[
            pltpu.VMEM((keys_count, inner), BF16),
            pltpu.VMEM((keys_count, inner), BF16),
            pltpu.VMEM((keys_count, LANES), BF16),
            pltpu.VMEM((tok_rows, LANES), BF16),
            pltpu.VMEM((inner, tok_rows), BF16),
        ],
        compiler_params=params(24),
        cost_estimate=pl.CostEstimate(flops=2 << 30, bytes_accessed=4 << 20, transcendentals=0),
        name="far",
    )(q, gates, mixed, w_out, *columns)


def solution(mesh):
    torus = Mesh(mesh.devices.reshape(mesh.shape["rep"], 4, 16, 2), REP_SEQ)
    return jax.shard_map(
        shards,
        mesh=torus,
        in_specs=(P(REP_SEQ, None), P(), P(), P(), P(), P(), P("rep")),
        out_specs=P(REP_SEQ, None),
        check_vma=False,
    )
```

```python
import jax
import jax.numpy as jnp
from jax import lax
from jax.experimental import pallas as pl
from jax.experimental.pallas import tpu as pltpu
from jax.sharding import Mesh
from jax.sharding import PartitionSpec as P

WINDOW = 128
REACH = 3
AX_X, AX_Z, AX_C = "seq_0", "seq_1", "seq_2"
SEQ = (AX_X, AX_Z, AX_C)
REP_SEQ = ("rep", AX_X, AX_Z, AX_C)
LANES = 128
NEG = -1e30
F32, BF16, I32 = jnp.float32, jnp.bfloat16, jnp.int32
NT = (((1,), (1,)), ((), ()))
TN = (((0,), (0,)), ((), ()))


def dot(a, b):
    return jnp.dot(a, b, preferred_element_type=F32)


def dot_nt(a, b):
    return lax.dot_general(a, b, NT, preferred_element_type=F32)


def iota(shape, dim):
    return lax.broadcasted_iota(I32, shape, dim)


def one_hot(condition):
    return jnp.where(condition, 1.0, 0.0).astype(BF16)


def half_lanes(rows):
    return iota((rows, LANES), 1) < LANES // 2


def token_classes(tok_rows, med_len):
    row, lane = iota((tok_rows, LANES), 0), iota((tok_rows, LANES), 1)
    wanted = 2 * (row // med_len) + jnp.where(row % med_len == med_len - 1, 1, 0)
    return one_hot(lane % (LANES // 2) == wanted)


def project_kernel(
    tok_hbm, w_hbm, cm_hbm, cc_hbm, kv_hbm, med_ref, pay_ref,
    tok_ref, w_buf, cm_ref, cc_ref, kv_ref, c_buf, sems, in_sems, out_sems,
):
    tok_rows = tok_ref.shape[0]
    _, _, med_len = cm_ref.shape
    coarse_len = cc_ref.shape[2]
    inner = kv_hbm.shape[1] // 2
    width = w_buf.shape[2]
    steps = w_buf.shape[0]
    fetches = [
        pltpu.make_async_copy(src, dst, in_sems.at[n])
        for n, (src, dst) in enumerate(((cm_hbm, cm_ref), (cc_hbm, cc_ref), (tok_hbm, tok_ref)))
    ]
    for fetch in fetches:
        fetch.start()
    copies = []
    for g in range(steps):
        columns = pl.ds(inner + g * width, width)
        copies.append(pltpu.make_async_copy(w_hbm.at[:, columns], w_buf.at[g], sems.at[g]))
        copies[-1].start()
    med_blocks = tok_rows // med_len
    coarse_blocks = tok_rows // coarse_len
    per = width // 64
    tile_up = one_hot(iota((med_len, tok_rows), 1) % med_len == iota((med_len, tok_rows), 0))
    own_block = iota((per * med_blocks, tok_rows), 0) % med_blocks == (
        iota((per * med_blocks, tok_rows), 1) // med_len
    )
    own_coarse = iota((8, tok_rows), 0) == iota((8, tok_rows), 1) // coarse_len
    count = c_buf.shape[0]
    total = pay_ref.shape[0]
    repeat = one_hot(iota((total, count), 0) % count == iota((total, count), 1))
    fetches[0].wait()
    fetches[1].wait()
    mixes = []
    for g in range(steps):
        side, first = (2 * g) // steps, (g % (steps // 2)) * per
        med_rows, coarse_rows = [], []
        for i in range(per):
            med_w = cm_ref[first + i].astype(F32)[side : side + 1, :]
            med_rows.append(jnp.broadcast_to(med_w, (med_blocks, med_len)))
            coarse_w = cc_ref[first + i].astype(F32)[side : side + 1, :]
            coarse_w = jnp.concatenate([coarse_w] * coarse_blocks, axis=1)
            coarse_rows.append(jnp.where(own_coarse, jnp.broadcast_to(coarse_w, (8, tok_rows)), 0.0))
        med_mix = dot(jnp.concatenate(med_rows, 0).astype(BF16), tile_up)
        med_mix = jnp.where(own_block, med_mix, 0.0)
        mixes.append(jnp.concatenate([med_mix] + coarse_rows, 0).astype(BF16))
    fetches[2].wait()
    stores = []
    for g in range(steps):
        copies[g].wait()
        rows = dot(tok_ref[...], w_buf[g]).astype(BF16)
        kv_ref[g] = rows
        stores.append(
            pltpu.make_async_copy(kv_ref.at[g], kv_hbm.at[:, pl.ds(g * width, width)], out_sems.at[g])
        )
        stores[-1].start()
        packed = dot(mixes[g], rows)
        med_head = iota((med_blocks, width), 1) // 64
        coarse_head = iota((8, width), 1) // 64
        med = jnp.zeros((med_blocks, width), F32)
        coarse = jnp.zeros((8, width), F32)
        for i in range(per):
            med = jnp.where(med_head == i, packed[i * med_blocks : (i + 1) * med_blocks], med)
            at = per * med_blocks + 8 * i
            coarse = jnp.where(coarse_head == i, packed[at : at + 8], coarse)
        med_ref[:, g * width : (g + 1) * width] = med.astype(BF16)
        for i in range(width // LANES):
            tile = g * (width // LANES) + i
            c_buf[tile * coarse_blocks : (tile + 1) * coarse_blocks, :] = coarse[
                :coarse_blocks, i * LANES : (i + 1) * LANES
            ]
    pay_ref[...] = dot(repeat, c_buf[...].astype(BF16)).astype(BF16)
    for store in stores:
        store.wait()


def values_up(tile, odd):
    eye = one_hot(iota((LANES, LANES), 0) == iota((LANES, LANES), 1))
    turned = dot_nt(eye, tile).astype(BF16)
    half = LANES // 2
    ones = jnp.ones((16, tile.shape[0]), BF16)
    return jnp.concatenate([turned[half * odd : half * (odd + 1)], ones], 0)


def window_kernel(
    tok_hbm, tail_ref, w_hbm, wg_ref, kv_hbm,
    q_ref, gate_ref, mix_ref, tok_ref, kv_ref, w_buf, tail_buf, sems, in_sems,
):
    tok_rows, _ = tok_ref.shape
    inner = kv_ref.shape[1] // 2
    width = w_buf.shape[2]
    steps = w_buf.shape[0]
    heads = gate_ref.shape[0] // 3
    half = LANES // 2
    fetch = pltpu.make_async_copy(tok_hbm, tok_ref, in_sems.at[0])
    fetch.start()
    copies = []
    for g in range(steps):
        copies.append(
            pltpu.make_async_copy(w_hbm.at[:, pl.ds(g * width, width)], w_buf.at[g], sems.at[g])
        )
        copies[-1].start()
    fetch_kv = pltpu.make_async_copy(kv_hbm, kv_ref, in_sems.at[1])
    fetch_kv.start()
    position = (lax.axis_index(AX_X) * lax.axis_size(AX_Z) + lax.axis_index(AX_Z)) * lax.axis_size(
        AX_C
    ) + lax.axis_index(AX_C)
    fetch.wait()
    gate_ref[...] = 1.0 / (1.0 + jnp.exp(-dot_nt(wg_ref[...], tok_ref[...])))
    for g in range(steps):
        copies[g].wait()
        lo = g * width
        if lo < inner:
            rows = dot(tok_ref[...], w_buf[g]).astype(BF16).astype(F32)
            q_ref[:, lo : lo + width] = (rows * (half**-0.5)).astype(BF16)
        else:
            tail_buf[:, lo - inner : lo - inner + width] = dot(tail_ref[...], w_buf[g]).astype(BF16)

    fetch_kv.wait()
    below = iota((WINDOW, WINDOW), 0) <= iota((WINDOW, WINDOW), 1)
    chunks = tok_rows // WINDOW
    first_bias = jnp.where(position == 0, NEG, 0.0)

    @pl.loop(0, heads // 2)
    def _(pair):
        at = pl.multiple_of(pair * LANES, LANES)
        at_v = pl.multiple_of(inner + pair * LANES, LANES)
        q_tile = q_ref[:, pl.ds(at, LANES)]
        keys = jnp.concatenate([tail_buf[:, pl.ds(at, LANES)], kv_ref[:, pl.ds(at, LANES)]], 0)
        values = jnp.concatenate([tail_buf[:, pl.ds(at_v, LANES)], kv_ref[:, pl.ds(at_v, LANES)]], 0)
        for odd in range(2):
            head = 2 * pair + odd
            mine_k = half_lanes(keys.shape[0]) if odd == 0 else ~half_lanes(keys.shape[0])
            k_ext = jnp.where(mine_k, keys, jnp.zeros_like(keys))
            merged = []
            for c in range(chunks):
                s = dot_nt(
                    k_ext[c * WINDOW : (c + 2) * WINDOW], q_tile[c * WINDOW : (c + 1) * WINDOW]
                )
                left, right = s[:WINDOW], s[WINDOW:]
                if c == 0:
                    left = left + first_bias
                merged.append(jnp.where(below, right, left))
            scores = jnp.concatenate(merged, 1)
            peak = jnp.max(scores, axis=0, keepdims=True)
            terms = jnp.exp(scores - peak).astype(BF16)
            v_up = values_up(values, odd)
            outs = []
            for c in range(chunks):
                part = terms[:, c * WINDOW : (c + 1) * WINDOW]
                zero = jnp.zeros_like(part)
                both_parts = jnp.concatenate(
                    [jnp.where(below, zero, part), jnp.where(below, part, zero)], 0
                )
                outs.append(dot(v_up[:, c * WINDOW : (c + 2) * WINDOW], both_parts))
            out = jnp.concatenate(outs, 1)
            factor = gate_ref[pl.ds(head, 1), :] / out[half : half + 1]
            mix_ref[pl.ds(pl.multiple_of(head * half, half), half), :] = out[:half] * factor


def medium_kernel(
    q_ref, gate_ref, old_hbm, far3_ref, far2_ref, far1_ref, med_ref, gid_ref, mix_ref,
    old_ref, bias_buf, hot_buf, sem,
):
    tok_rows, inner = q_ref.shape
    heads = gate_ref.shape[0] // 3
    med_blocks = med_ref.shape[0]
    near = (REACH + 1) * med_blocks
    half = LANES // 2
    fetch = pltpu.make_async_copy(old_hbm, old_ref, sem)
    fetch.start()
    position = (lax.axis_index(AX_X) * lax.axis_size(AX_Z) + lax.axis_index(AX_Z)) * lax.axis_size(
        AX_C
    ) + lax.axis_index(AX_C)
    hot_buf[...] = token_classes(tok_rows, tok_rows // med_blocks)

    first = (position - REACH) * med_blocks
    padded = first + near
    row = padded // LANES - 1
    offset = padded % LANES
    low = gid_ref[pl.ds(jnp.maximum(row, 0), 1), :]
    high = gid_ref[pl.ds(jnp.minimum(row + 1, gid_ref.shape[0] - 1), 1), :]
    lane = iota((1, LANES), 1)
    both = jnp.where(lane >= offset, low, high)
    near_groups = pltpu.roll(jnp.broadcast_to(both, (8, LANES)), (LANES - offset) % LANES, 1)[:1]
    near_groups = jnp.where(lane + first >= 0, near_groups, -1).astype(F32)
    spread = jnp.broadcast_to(near_groups, (near, LANES)).astype(BF16)
    i0, i1 = iota((near, LANES), 0), iota((near, LANES), 1)
    key_group = dot_nt(one_hot(i0 == i1), spread)
    own = (i1 % half) // 2 + REACH * med_blocks
    token_group = dot(spread, one_hot(i0 == own))
    visible = (key_group == token_group) & ((i0 < own) | ((i0 == own) & (i1 % 2 == 1)))
    bias_buf[...] = jnp.where(visible, 0.0, NEG).astype(BF16)
    fetch.wait()

    @pl.loop(0, heads // 2)
    def _(pair):
        at = pl.multiple_of(pair * LANES, LANES)
        at_v = pl.multiple_of(inner + pair * LANES, LANES)
        q_tile = q_ref[:, pl.ds(at, LANES)]
        blocks = (far3_ref, far2_ref, far1_ref, med_ref)
        med_k = jnp.concatenate([b[:, pl.ds(at, LANES)] for b in blocks], 0)
        med_v = jnp.concatenate([b[:, pl.ds(at_v, LANES)] for b in blocks], 0)
        for odd in range(2):
            head = 2 * pair + odd
            mine = half_lanes(tok_rows) if odd == 0 else ~half_lanes(tok_rows)
            q_ext = jnp.where(mine, q_tile, hot_buf[...])
            mine_m = half_lanes(near) if odd == 0 else ~half_lanes(near)
            scores = dot_nt(jnp.where(mine_m, med_k, bias_buf[...]), q_ext)
            peak = jnp.maximum(jnp.max(scores, axis=0, keepdims=True), 0.0)
            terms = jnp.exp(scores - peak).astype(BF16)
            out = dot(values_up(med_v, odd), terms)
            factor = gate_ref[pl.ds(heads + head, 1), :] / (jnp.exp(-peak) + out[half : half + 1])
            rows = pl.ds(pl.multiple_of(head * half, half), half)
            mix_ref[rows, :] = old_ref[rows, :] + out[:half] * factor


def far_kernel(
    q_ref, gate_ref, mix_ref, w_hbm, *refs
):
    pieces, scratch = refs[:-8], refs[-8:]
    out_ref, keys_buf, values_buf, bias_buf, hot_buf, mixed_buf, w_ref, sem = scratch
    fetch = pltpu.make_async_copy(w_hbm, w_ref, sem)
    fetch.start()
    tok_rows, inner = q_ref.shape
    heads = gate_ref.shape[0] // 3
    half = LANES // 2
    tiles = inner // LANES
    total = pieces[0].shape[0]
    zs = lax.axis_size(AX_Z)
    count = total // zs
    each = total // (2 * tiles)
    per = each // zs
    pos_x, pos_z, pos_c = lax.axis_index(AX_X), lax.axis_index(AX_Z), lax.axis_index(AX_C)
    xs, cs = lax.axis_size(AX_X), lax.axis_size(AX_C)
    hot_buf[...] = token_classes(tok_rows, 16)

    r0, r1 = iota((total, total), 0), iota((total, total), 1)
    source = ((r0 % each) // per) * count + (r0 // each) * per + r0 % per
    turn = one_hot(source == r1)
    sorted_rows = dot(turn, jnp.concatenate([p[...] for p in pieces], 1)).astype(BF16)
    lane = iota((each, LANES), 1) % half
    row = iota((each, LANES), 0)
    position = (pos_x * zs + pos_z) * cs + pos_c
    seen = per * position + jnp.where(lane >= half // per - 1, 1, 0) + jnp.where(lane == half - 1, 1, 0)
    for n in range(len(pieces)):
        for t in range(tiles):
            block = sorted_rows[t * each : (t + 1) * each, n * LANES : (n + 1) * LANES]
            keys_buf[n * each : (n + 1) * each, t * LANES : (t + 1) * LANES] = block
            block = sorted_rows[(tiles + t) * each : (tiles + t + 1) * each, n * LANES : (n + 1) * LANES]
            values_buf[n * each : (n + 1) * each, t * LANES : (t + 1) * LANES] = block
        from_x = lax.rem(pos_x + xs - n % xs, xs)
        from_c = lax.rem(pos_c + n // xs, cs)
        index = ((from_x * zs + row // per) * cs + from_c) * per + row % per
        bias_buf[n * each : (n + 1) * each, :] = jnp.where(index < seen, 0.0, NEG).astype(BF16)

    keys_count = keys_buf.shape[0]

    @pl.loop(0, tiles)
    def _(pair):
        at = pl.multiple_of(pair * LANES, LANES)
        q_tile = q_ref[:, pl.ds(at, LANES)]
        keys = keys_buf[:, pl.ds(at, LANES)]
        values = values_buf[:, pl.ds(at, LANES)]
        for odd in range(2):
            head = 2 * pair + odd
            mine = half_lanes(tok_rows) if odd == 0 else ~half_lanes(tok_rows)
            q_ext = jnp.where(mine, q_tile, hot_buf[...])
            mine_k = half_lanes(keys_count) if odd == 0 else ~half_lanes(keys_count)
            scores = dot_nt(jnp.where(mine_k, keys, bias_buf[...]), q_ext)
            peak = jnp.maximum(jnp.max(scores, axis=0, keepdims=True), 0.0)
            terms = jnp.exp(scores - peak).astype(BF16)
            out = dot(values_up(values, odd), terms)
            factor = gate_ref[pl.ds(2 * heads + head, 1), :] / (jnp.exp(-peak) + out[half : half + 1])
            rows = pl.ds(pl.multiple_of(head * half, half), half)
            mixed_buf[rows, :] = (mix_ref[rows, :] + out[:half] * factor).astype(BF16)

    fetch.wait()
    out_ref[...] = lax.dot_general(
        mixed_buf[...], w_ref[...], TN, preferred_element_type=F32
    ).astype(BF16)


def shifted(block, axis, distance):
    size = lax.axis_size(axis)
    return lax.ppermute(block, axis, [(i - distance, i) for i in range(distance, size)])


def turned(block, axis, distance):
    size = lax.axis_size(axis)
    return lax.ppermute(block, axis, [(i, (i + distance) % size) for i in range(size)])


VMEM = pl.BlockSpec(memory_space=pltpu.VMEM)
HBM = pl.BlockSpec(memory_space=pltpu.HBM)


def params(kib):
    return pltpu.CompilerParams(vmem_limit_bytes=kib << 10)


def cost(flops, moved):
    return pl.CostEstimate(flops=int(flops), bytes_accessed=int(moved), transcendentals=0)


def shards(tokens, w_qkv, w_gate, w_out, cmp_med, cmp_coarse, group_id):
    tok_rows, depth = tokens.shape
    heads, med_len, coarse_len = cmp_med.shape[1], cmp_med.shape[2], cmp_coarse.shape[2]
    inner = w_out.shape[0]
    width = 256
    med_blocks = tok_rows // med_len
    coarse_blocks = tok_rows // coarse_len
    zs = lax.axis_size(AX_Z)
    count = coarse_blocks * 2 * inner // LANES
    tail = shifted(tokens[tok_rows - WINDOW :], SEQ, 1)

    kv_steps = 2 * inner // width
    cmp_med, cmp_coarse = cmp_med.transpose(1, 0, 2), cmp_coarse.transpose(1, 0, 2)
    kv, med, payload = pl.pallas_call(
        project_kernel,
        out_shape=(
            jax.ShapeDtypeStruct((tok_rows, 2 * inner), BF16),
            jax.ShapeDtypeStruct((med_blocks, 2 * inner), BF16),
            jax.ShapeDtypeStruct((zs * count, LANES), BF16),
        ),
        in_specs=[HBM] * 4,
        out_specs=(HBM, VMEM, VMEM),
        scratch_shapes=[
            pltpu.VMEM(tokens.shape, BF16),
            pltpu.VMEM((kv_steps, depth, width), BF16),
            pltpu.VMEM(cmp_med.shape, BF16),
            pltpu.VMEM(cmp_coarse.shape, BF16),
            pltpu.VMEM((kv_steps, tok_rows, width), BF16),
            pltpu.VMEM((count, LANES), F32),
            pltpu.SemaphoreType.DMA((kv_steps,)),
            pltpu.SemaphoreType.DMA((3,)),
            pltpu.SemaphoreType.DMA((kv_steps,)),
        ],
        compiler_params=params(62100),
        cost_estimate=cost(4e9, 4e6),
        name="project",
    )(tokens, w_qkv, cmp_med, cmp_coarse)

    column = lax.all_to_all(payload, AX_Z, 0, 0, tiled=True)
    far1, far2, far3 = (shifted(med, SEQ, k) for k in (1, 2, 3))

    all_steps = 3 * inner // width
    q, gates, mixed = pl.pallas_call(
        window_kernel,
        out_shape=(
            jax.ShapeDtypeStruct((tok_rows, inner), BF16),
            jax.ShapeDtypeStruct((3 * heads, tok_rows), F32),
            jax.ShapeDtypeStruct((inner, tok_rows), F32),
        ),
        in_specs=[HBM, VMEM, HBM, VMEM, HBM],
        out_specs=(VMEM, VMEM, VMEM),
        scratch_shapes=[
            pltpu.VMEM(tokens.shape, BF16),
            pltpu.VMEM((tok_rows, 2 * inner), BF16),
            pltpu.VMEM((all_steps, depth, width), BF16),
            pltpu.VMEM((WINDOW, 2 * inner), BF16),
            pltpu.SemaphoreType.DMA((all_steps,)),
            pltpu.SemaphoreType.DMA((2,)),
        ],
        compiler_params=params(54000),
        cost_estimate=cost(8e9, 8e6),
        name="window",
    )(tokens, tail, w_qkv, w_gate.T, kv)

    columns = [column] + [turned(column, AX_X, k) for k in range(1, lax.axis_size(AX_X))]
    mixed = pl.pallas_call(
        medium_kernel,
        out_shape=jax.ShapeDtypeStruct((inner, tok_rows), F32),
        in_specs=[VMEM, VMEM, HBM] + [VMEM] * 5,
        out_specs=VMEM,
        scratch_shapes=[
            pltpu.VMEM((inner, tok_rows), F32),
            pltpu.VMEM(((REACH + 1) * med_blocks, LANES), BF16),
            pltpu.VMEM((tok_rows, LANES), BF16),
            pltpu.SemaphoreType.DMA,
        ],
        compiler_params=params(48000),
        cost_estimate=cost(4e9, 4e6),
        name="medium",
    )(q, gates, mixed, far3, far2, far1, med, group_id.reshape(-1, LANES))
    columns += [turned(c, AX_C, 1) for c in columns]
    keys_count = coarse_blocks * lax.axis_size(SEQ)
    return pl.pallas_call(
        far_kernel,
        out_shape=jax.ShapeDtypeStruct((tok_rows, inner), BF16),
        in_specs=[VMEM] * 3 + [HBM] + [VMEM] * len(columns),
        out_specs=VMEM,
        scratch_shapes=[
            pltpu.VMEM((keys_count, inner), BF16),
            pltpu.VMEM((keys_count, inner), BF16),
            pltpu.VMEM((keys_count, LANES), BF16),
            pltpu.VMEM((tok_rows, LANES), BF16),
            pltpu.VMEM((inner, tok_rows), BF16),
            pltpu.VMEM(w_out.shape, BF16),
            pltpu.SemaphoreType.DMA,
        ],
        compiler_params=params(48000),
        cost_estimate=cost(4e9, 4e6),
        name="far",
    )(q, gates, mixed, w_out, *columns)


def solution(mesh):
    torus = Mesh(mesh.devices.reshape(mesh.shape["rep"], 4, 16, 2), REP_SEQ)

    return jax.shard_map(
        shards,
        mesh=torus,
        in_specs=(P(REP_SEQ, None), P(), P(), P(), P(), P(), P("rep")),
        out_specs=P(REP_SEQ, None),
        check_vma=False,
    )
```

```python
import functools

import jax
import jax.numpy as jnp
from jax import lax
from jax.experimental import pallas as pl
from jax.experimental.pallas import tpu as pltpu
from jax.sharding import Mesh
from jax.sharding import PartitionSpec as P

WINDOW = 128
REACH = 3
AX_X, AX_Z, AX_C = "seq_0", "seq_1", "seq_2"
SEQ = (AX_X, AX_Z, AX_C)
REP_SEQ = ("rep", AX_X, AX_Z, AX_C)
LANES = 128
NEG = -1e30
F32, BF16, I32 = jnp.float32, jnp.bfloat16, jnp.int32
NT = (((1,), (1,)), ((), ()))
TN = (((0,), (0,)), ((), ()))


def dot(a, b):
    return jnp.dot(a, b, preferred_element_type=F32)


def dot_nt(a, b):
    return lax.dot_general(a, b, NT, preferred_element_type=F32)


def iota(shape, dim):
    return lax.broadcasted_iota(I32, shape, dim)


def one_hot(condition):
    return jnp.where(condition, 1.0, 0.0).astype(BF16)


def half_lanes(rows):
    return iota((rows, LANES), 1) < LANES // 2


def token_classes(tok_rows, med_len):
    row, lane = iota((tok_rows, LANES), 0), iota((tok_rows, LANES), 1)
    wanted = 2 * (row // med_len) + jnp.where(row % med_len == med_len - 1, 1, 0)
    return one_hot(lane % (LANES // 2) == wanted)


def project_kernel(
    tok_hbm, w_hbm, cm_hbm, cc_hbm, kv_hbm, edge_ref, med_ref, pay_ref,
    tok_ref, w_buf, cm_ref, cc_ref, kv_ref, c_buf, sems, in_sems, out_sems,
):
    tok_rows = tok_ref.shape[0]
    _, _, med_len = cm_ref.shape
    coarse_len = cc_ref.shape[2]
    inner = kv_hbm.shape[1] // 2
    width = w_buf.shape[2]
    steps = w_buf.shape[0]
    fetches = [
        pltpu.make_async_copy(src, dst, in_sems.at[n])
        for n, (src, dst) in enumerate(((cm_hbm, cm_ref), (cc_hbm, cc_ref), (tok_hbm, tok_ref)))
    ]
    for fetch in fetches:
        fetch.start()
    copies = []
    for g in range(steps):
        columns = pl.ds(inner + g * width, width)
        copies.append(pltpu.make_async_copy(w_hbm.at[:, columns], w_buf.at[g], sems.at[g]))
        copies[-1].start()
    med_blocks = tok_rows // med_len
    coarse_blocks = tok_rows // coarse_len
    per = width // 64
    tile_up = one_hot(iota((med_len, tok_rows), 1) % med_len == iota((med_len, tok_rows), 0))
    own_block = iota((per * med_blocks, tok_rows), 0) % med_blocks == (
        iota((per * med_blocks, tok_rows), 1) // med_len
    )
    own_coarse = iota((8, tok_rows), 0) == iota((8, tok_rows), 1) // coarse_len
    count = c_buf.shape[0]
    total = pay_ref.shape[0]
    repeat = one_hot(iota((total, count), 0) % count == iota((total, count), 1))
    fetches[0].wait()
    fetches[1].wait()
    mixes = []
    for g in range(steps):
        side, first = (2 * g) // steps, (g % (steps // 2)) * per
        med_rows, coarse_rows = [], []
        for i in range(per):
            med_w = cm_ref[first + i].astype(F32)[side : side + 1, :]
            med_rows.append(jnp.broadcast_to(med_w, (med_blocks, med_len)))
            coarse_w = cc_ref[first + i].astype(F32)[side : side + 1, :]
            coarse_w = jnp.concatenate([coarse_w] * coarse_blocks, axis=1)
            coarse_rows.append(jnp.where(own_coarse, jnp.broadcast_to(coarse_w, (8, tok_rows)), 0.0))
        med_mix = dot(jnp.concatenate(med_rows, 0).astype(BF16), tile_up)
        med_mix = jnp.where(own_block, med_mix, 0.0)
        mixes.append(jnp.concatenate([med_mix] + coarse_rows, 0).astype(BF16))
    fetches[2].wait()
    stores = []
    for g in range(steps):
        copies[g].wait()
        rows = dot(tok_ref[...], w_buf[g]).astype(BF16)
        kv_ref[g] = rows
        stores.append(
            pltpu.make_async_copy(kv_ref.at[g], kv_hbm.at[:, pl.ds(g * width, width)], out_sems.at[g])
        )
        stores[-1].start()
        packed = dot(mixes[g], rows)
        med_head = iota((med_blocks, width), 1) // 64
        coarse_head = iota((8, width), 1) // 64
        med = jnp.zeros((med_blocks, width), F32)
        coarse = jnp.zeros((8, width), F32)
        for i in range(per):
            med = jnp.where(med_head == i, packed[i * med_blocks : (i + 1) * med_blocks], med)
            at = per * med_blocks + 8 * i
            coarse = jnp.where(coarse_head == i, packed[at : at + 8], coarse)
        med_ref[:, g * width : (g + 1) * width] = med.astype(BF16)
        edge_ref[WINDOW:, g * width : (g + 1) * width] = med.astype(BF16)
        edge_ref[:WINDOW, g * width : (g + 1) * width] = rows[tok_rows - WINDOW :]
        for i in range(width // LANES):
            tile = g * (width // LANES) + i
            c_buf[tile * coarse_blocks : (tile + 1) * coarse_blocks, :] = coarse[
                :coarse_blocks, i * LANES : (i + 1) * LANES
            ]
    pay_ref[...] = dot(repeat, c_buf[...].astype(BF16)).astype(BF16)
    for store in stores:
        store.wait()


def values_up(tile, odd):
    eye = one_hot(iota((LANES, LANES), 0) == iota((LANES, LANES), 1))
    turned = dot_nt(eye, tile).astype(BF16)
    half = LANES // 2
    ones = jnp.ones((16, tile.shape[0]), BF16)
    return jnp.concatenate([turned[half * odd : half * (odd + 1)], ones], 0)


def device_position():
    return (lax.axis_index(AX_X) * lax.axis_size(AX_Z) + lax.axis_index(AX_Z)) * lax.axis_size(
        AX_C
    ) + lax.axis_index(AX_C)


def window_scores(keys, q_tile, odd, first_bias=None):
    below = iota((WINDOW, WINDOW), 0) <= iota((WINDOW, WINDOW), 1)
    mine = half_lanes(keys.shape[0]) if odd == 0 else ~half_lanes(keys.shape[0])
    k_ext = jnp.where(mine, keys, jnp.zeros_like(keys))
    merged = []
    for c in range(q_tile.shape[0] // WINDOW):
        s = dot_nt(k_ext[c * WINDOW : (c + 2) * WINDOW], q_tile[c * WINDOW : (c + 1) * WINDOW])
        left, right = s[:WINDOW], s[WINDOW:]
        if first_bias is not None:
            left = left + first_bias
        merged.append(jnp.where(below, right, left))
    return jnp.concatenate(merged, 1)


def window_values(scores, v_up, gate):
    below = iota((WINDOW, WINDOW), 0) <= iota((WINDOW, WINDOW), 1)
    half = LANES // 2
    terms = jnp.exp(scores - jnp.max(scores, axis=0, keepdims=True)).astype(BF16)
    outs = []
    for c in range(scores.shape[1] // WINDOW):
        part = terms[:, c * WINDOW : (c + 1) * WINDOW]
        zero = jnp.zeros_like(part)
        both = jnp.concatenate([jnp.where(below, zero, part), jnp.where(below, part, zero)], 0)
        outs.append(dot(v_up[:, c * WINDOW : (c + 2) * WINDOW], both))
    out = jnp.concatenate(outs, 1)
    return out[:half] * (gate / out[half : half + 1])


def window_kernel(early, tok_hbm, w_hbm, wg_ref, kv_hbm, *refs):
    (
        q_hbm, gate_hbm, mix_hbm,
        tok_ref, kv_ref, w_buf, q_ref, gate_ref, mix_ref, sems, in_sems, out_sems,
    ) = refs[-12:]
    low = lax.axis_index(AX_Z) < lax.axis_size(AX_Z) // 2

    @pl.when(low if early else jnp.logical_not(low))
    def _():
        inner = kv_ref.shape[1] // 2
        steps, _, width = w_buf.shape
        heads = gate_ref.shape[0] // 3
        half = LANES // 2
        fetch = pltpu.make_async_copy(tok_hbm, tok_ref, in_sems.at[0])
        fetch.start()
        copies = []
        for g in range(steps):
            copies.append(
                pltpu.make_async_copy(w_hbm.at[:, pl.ds(g * width, width)], w_buf.at[g], sems.at[g])
            )
            copies[-1].start()
        fetch_kv = pltpu.make_async_copy(kv_hbm, kv_ref, in_sems.at[1])
        fetch_kv.start()
        fetch.wait()
        gate_ref[...] = 1.0 / (1.0 + jnp.exp(-dot_nt(wg_ref[...], tok_ref[...])))
        for g in range(steps):
            copies[g].wait()
            rows = dot(tok_ref[...], w_buf[g]).astype(BF16).astype(F32)
            q_ref[:, g * width : (g + 1) * width] = (rows * (half**-0.5)).astype(BF16)
        fetch_kv.wait()

        @pl.loop(0, heads // 2)
        def _(pair):
            at = pl.multiple_of(pair * LANES, LANES)
            at_v = pl.multiple_of(inner + pair * LANES, LANES)
            q_tile = q_ref[WINDOW:, pl.ds(at, LANES)]
            keys = kv_ref[:, pl.ds(at, LANES)]
            values = kv_ref[:, pl.ds(at_v, LANES)]
            for odd in range(2):
                head = 2 * pair + odd
                scores = window_scores(keys, q_tile, odd)
                mix_ref[pl.ds(pl.multiple_of(head * half, half), half), :] = window_values(
                    scores, values_up(values, odd), gate_ref[pl.ds(head, 1), :][:, WINDOW:]
                )

        stores = [
            pltpu.make_async_copy(src, dst, out_sems.at[n])
            for n, (src, dst) in enumerate(((q_ref, q_hbm), (gate_ref, gate_hbm), (mix_ref, mix_hbm)))
        ]
        for store in stores:
            store.start()
        for store in stores:
            store.wait()


def medium_kernel(
    q_hbm, gate_hbm, old_hbm, kv_hbm, far3_ref, far2_ref, edge_ref, med_ref, gid_ref, mix_ref,
    q_ref, gate_ref, old_ref, kv_ref, bias_buf, hot_buf, sems,
):
    tok_rows, inner = q_ref.shape
    heads = gate_ref.shape[0] // 3
    med_blocks = med_ref.shape[0]
    near = (REACH + 1) * med_blocks
    half = LANES // 2
    moves = ((q_hbm, q_ref), (gate_hbm, gate_ref), (kv_hbm.at[pl.ds(0, WINDOW)], kv_ref), (old_hbm, old_ref))
    fetches = [pltpu.make_async_copy(src, dst, sems.at[n]) for n, (src, dst) in enumerate(moves)]
    for fetch in fetches:
        fetch.start()
    position = device_position()
    hot_buf[...] = token_classes(tok_rows, tok_rows // med_blocks)

    first = (position - REACH) * med_blocks
    padded = first + near
    row = padded // LANES - 1
    offset = padded % LANES
    low = gid_ref[pl.ds(jnp.maximum(row, 0), 1), :]
    high = gid_ref[pl.ds(jnp.minimum(row + 1, gid_ref.shape[0] - 1), 1), :]
    lane = iota((1, LANES), 1)
    both = jnp.where(lane >= offset, low, high)
    near_groups = pltpu.roll(jnp.broadcast_to(both, (8, LANES)), (LANES - offset) % LANES, 1)[:1]
    near_groups = jnp.where(lane + first >= 0, near_groups, -1).astype(F32)
    spread = jnp.broadcast_to(near_groups, (near, LANES)).astype(BF16)
    i0, i1 = iota((near, LANES), 0), iota((near, LANES), 1)
    key_group = dot_nt(one_hot(i0 == i1), spread)
    own = (i1 % half) // 2 + REACH * med_blocks
    token_group = dot(spread, one_hot(i0 == own))
    visible = (key_group == token_group) & ((i0 < own) | ((i0 == own) & (i1 % 2 == 1)))
    bias_buf[...] = jnp.where(visible, 0.0, NEG).astype(BF16)
    first_bias = jnp.where(position == 0, NEG, 0.0)
    for fetch in fetches:
        fetch.wait()

    @pl.loop(0, heads // 2)
    def _(pair):
        at = pl.multiple_of(pair * LANES, LANES)
        at_v = pl.multiple_of(inner + pair * LANES, LANES)
        q_tile = q_ref[:, pl.ds(at, LANES)]
        keys = jnp.concatenate([edge_ref[:WINDOW, pl.ds(at, LANES)], kv_ref[:, pl.ds(at, LANES)]], 0)
        values = jnp.concatenate(
            [edge_ref[:WINDOW, pl.ds(at_v, LANES)], kv_ref[:, pl.ds(at_v, LANES)]], 0
        )
        blocks = (far3_ref, far2_ref, edge_ref.at[pl.ds(WINDOW, med_blocks)], med_ref)
        med_k = jnp.concatenate([b[:, pl.ds(at, LANES)] for b in blocks], 0)
        med_v = jnp.concatenate([b[:, pl.ds(at_v, LANES)] for b in blocks], 0)
        for odd in range(2):
            head = 2 * pair + odd
            mine = half_lanes(tok_rows) if odd == 0 else ~half_lanes(tok_rows)
            q_ext = jnp.where(mine, q_tile, hot_buf[...])
            mine_m = half_lanes(near) if odd == 0 else ~half_lanes(near)
            scores = dot_nt(jnp.where(mine_m, med_k, bias_buf[...]), q_ext)
            rim_scores = window_scores(keys, q_tile[:WINDOW], odd, first_bias)
            peak = jnp.maximum(jnp.max(scores, axis=0, keepdims=True), 0.0)
            terms = jnp.exp(scores - peak).astype(BF16)
            out = dot(values_up(med_v, odd), terms)
            factor = gate_ref[pl.ds(heads + head, 1), :] / (jnp.exp(-peak) + out[half : half + 1])
            rim = window_values(rim_scores, values_up(values, odd), gate_ref[pl.ds(head, 1), :][:, :WINDOW])
            rows = pl.ds(pl.multiple_of(head * half, half), half)
            mix_ref[rows, :] = jnp.concatenate([rim, old_ref[rows, :]], 1) + out[:half] * factor


def far_kernel(
    q_hbm, gate_hbm, mix_ref, w_hbm, *refs
):
    pieces, scratch = refs[:-10], refs[-10:]
    out_ref, keys_buf, values_buf, bias_buf, hot_buf, mixed_buf, w_ref, q_ref, gate_ref, sems = scratch
    moves = ((q_hbm, q_ref), (gate_hbm, gate_ref), (w_hbm, w_ref))
    fetches = [pltpu.make_async_copy(src, dst, sems.at[n]) for n, (src, dst) in enumerate(moves)]
    for fetch in fetches:
        fetch.start()
    tok_rows, inner = q_ref.shape
    heads = gate_ref.shape[0] // 3
    half = LANES // 2
    tiles = inner // LANES
    total = pieces[0].shape[0]
    zs = lax.axis_size(AX_Z)
    count = total // zs
    each = total // (2 * tiles)
    per = each // zs
    pos_x, pos_z, pos_c = lax.axis_index(AX_X), lax.axis_index(AX_Z), lax.axis_index(AX_C)
    xs, cs = lax.axis_size(AX_X), lax.axis_size(AX_C)
    hot_buf[...] = token_classes(tok_rows, 16)

    r0, r1 = iota((total, total), 0), iota((total, total), 1)
    source = ((r0 % each) // per) * count + (r0 // each) * per + r0 % per
    turn = one_hot(source == r1)
    sorted_rows = dot(turn, jnp.concatenate([p[...] for p in pieces], 1)).astype(BF16)
    lane = iota((each, LANES), 1) % half
    row = iota((each, LANES), 0)
    position = (pos_x * zs + pos_z) * cs + pos_c
    seen = per * position + jnp.where(lane >= half // per - 1, 1, 0) + jnp.where(lane == half - 1, 1, 0)
    for n in range(len(pieces)):
        for t in range(tiles):
            block = sorted_rows[t * each : (t + 1) * each, n * LANES : (n + 1) * LANES]
            keys_buf[n * each : (n + 1) * each, t * LANES : (t + 1) * LANES] = block
            block = sorted_rows[(tiles + t) * each : (tiles + t + 1) * each, n * LANES : (n + 1) * LANES]
            values_buf[n * each : (n + 1) * each, t * LANES : (t + 1) * LANES] = block
        from_x = lax.rem(pos_x + xs - n % xs, xs)
        from_c = lax.rem(pos_c + n // xs, cs)
        index = ((from_x * zs + row // per) * cs + from_c) * per + row % per
        bias_buf[n * each : (n + 1) * each, :] = jnp.where(index < seen, 0.0, NEG).astype(BF16)

    keys_count = keys_buf.shape[0]
    fetches[0].wait()
    fetches[1].wait()

    @pl.loop(0, tiles)
    def _(pair):
        at = pl.multiple_of(pair * LANES, LANES)
        q_tile = q_ref[:, pl.ds(at, LANES)]
        keys = keys_buf[:, pl.ds(at, LANES)]
        values = values_buf[:, pl.ds(at, LANES)]
        for odd in range(2):
            head = 2 * pair + odd
            mine = half_lanes(tok_rows) if odd == 0 else ~half_lanes(tok_rows)
            q_ext = jnp.where(mine, q_tile, hot_buf[...])
            mine_k = half_lanes(keys_count) if odd == 0 else ~half_lanes(keys_count)
            scores = dot_nt(jnp.where(mine_k, keys, bias_buf[...]), q_ext)
            peak = jnp.maximum(jnp.max(scores, axis=0, keepdims=True), 0.0)
            terms = jnp.exp(scores - peak).astype(BF16)
            out = dot(values_up(values, odd), terms)
            factor = gate_ref[pl.ds(2 * heads + head, 1), :] / (jnp.exp(-peak) + out[half : half + 1])
            rows = pl.ds(pl.multiple_of(head * half, half), half)
            mixed_buf[rows, :] = (mix_ref[rows, :] + out[:half] * factor).astype(BF16)

    fetches[2].wait()
    out_ref[...] = lax.dot_general(
        mixed_buf[...], w_ref[...], TN, preferred_element_type=F32
    ).astype(BF16)


def shifted(block, axis, distance):
    size = lax.axis_size(axis)
    return lax.ppermute(block, axis, [(i - distance, i) for i in range(distance, size)])


def turned(block, axis, distance):
    size = lax.axis_size(axis)
    return lax.ppermute(block, axis, [(i, (i + distance) % size) for i in range(size)])


VMEM = pl.BlockSpec(memory_space=pltpu.VMEM)
HBM = pl.BlockSpec(memory_space=pltpu.HBM)


def params(kib):
    return pltpu.CompilerParams(vmem_limit_bytes=kib << 10)


def cost(flops, moved):
    return pl.CostEstimate(flops=int(flops), bytes_accessed=int(moved), transcendentals=0)


def shards(tokens, w_qkv, w_gate, w_out, cmp_med, cmp_coarse, group_id):
    tok_rows, depth = tokens.shape
    heads, med_len, coarse_len = cmp_med.shape[1], cmp_med.shape[2], cmp_coarse.shape[2]
    inner = w_out.shape[0]
    width = 256
    med_blocks = tok_rows // med_len
    coarse_blocks = tok_rows // coarse_len
    zs = lax.axis_size(AX_Z)
    count = coarse_blocks * 2 * inner // LANES
    kv_steps = 2 * inner // width
    cmp_med, cmp_coarse = cmp_med.transpose(1, 0, 2), cmp_coarse.transpose(1, 0, 2)
    kv, edge, med, payload = pl.pallas_call(
        project_kernel,
        out_shape=(
            jax.ShapeDtypeStruct((tok_rows, 2 * inner), BF16),
            jax.ShapeDtypeStruct((WINDOW + med_blocks, 2 * inner), BF16),
            jax.ShapeDtypeStruct((med_blocks, 2 * inner), BF16),
            jax.ShapeDtypeStruct((zs * count, LANES), BF16),
        ),
        in_specs=[HBM] * 4,
        out_specs=(HBM, VMEM, VMEM, VMEM),
        scratch_shapes=[
            pltpu.VMEM(tokens.shape, BF16),
            pltpu.VMEM((kv_steps, depth, width), BF16),
            pltpu.VMEM(cmp_med.shape, BF16),
            pltpu.VMEM(cmp_coarse.shape, BF16),
            pltpu.VMEM((kv_steps, tok_rows, width), BF16),
            pltpu.VMEM((count, LANES), F32),
            pltpu.SemaphoreType.DMA((kv_steps,)),
            pltpu.SemaphoreType.DMA((3,)),
            pltpu.SemaphoreType.DMA((kv_steps,)),
        ],
        compiler_params=params(58000),
        cost_estimate=cost(4e9, 4e6),
        name="project",
    )(tokens, w_qkv, cmp_med, cmp_coarse)

    q_steps = inner // width
    window_shapes = (
        jax.ShapeDtypeStruct((tok_rows, inner), BF16),
        jax.ShapeDtypeStruct((3 * heads, tok_rows), F32),
        jax.ShapeDtypeStruct((inner, tok_rows - WINDOW), F32),
    )

    def window(early, *given):
        return pl.pallas_call(
            functools.partial(window_kernel, early),
            out_shape=window_shapes,
            in_specs=[HBM, HBM, VMEM, HBM] + [HBM] * len(given),
            out_specs=(HBM, HBM, HBM),
            input_output_aliases={4 + n: n for n in range(len(given))},
            scratch_shapes=[
                pltpu.VMEM(tokens.shape, BF16),
                pltpu.VMEM((tok_rows, 2 * inner), BF16),
                pltpu.VMEM((q_steps, depth, width), BF16),
                *(pltpu.VMEM(o.shape, o.dtype) for o in window_shapes),
                pltpu.SemaphoreType.DMA((q_steps,)),
                pltpu.SemaphoreType.DMA((2,)),
                pltpu.SemaphoreType.DMA((3,)),
            ],
            compiler_params=params(54000),
            cost_estimate=cost(8e9, 8e6),
            name="window",
        )(tokens, w_qkv, w_gate.T, kv, *given)

    parts = window(True)
    column = lax.all_to_all(payload, AX_Z, 0, 0, tiled=True)
    edge1, far2, far3 = shifted(edge, SEQ, 1), shifted(med, SEQ, 2), shifted(med, SEQ, 3)
    q, gates, mixed = window(False, *parts)
    columns = [column] + [turned(column, AX_X, k) for k in range(1, lax.axis_size(AX_X))]
    mixed = pl.pallas_call(
        medium_kernel,
        out_shape=jax.ShapeDtypeStruct((inner, tok_rows), F32),
        in_specs=[HBM] * 4 + [VMEM] * 5,
        out_specs=VMEM,
        scratch_shapes=[
            *(pltpu.VMEM(o.shape, o.dtype) for o in window_shapes),
            pltpu.VMEM((WINDOW, 2 * inner), BF16),
            pltpu.VMEM(((REACH + 1) * med_blocks, LANES), BF16),
            pltpu.VMEM((tok_rows, LANES), BF16),
            pltpu.SemaphoreType.DMA((4,)),
        ],
        compiler_params=params(48000),
        cost_estimate=cost(4e9, 4e6),
        name="medium",
    )(q, gates, mixed, kv, far3, far2, edge1, med, group_id.reshape(-1, LANES))
    columns += [turned(c, AX_C, 1) for c in columns]
    keys_count = coarse_blocks * lax.axis_size(SEQ)
    return pl.pallas_call(
        far_kernel,
        out_shape=jax.ShapeDtypeStruct((tok_rows, inner), BF16),
        in_specs=[HBM, HBM, VMEM, HBM] + [VMEM] * len(columns),
        out_specs=VMEM,
        scratch_shapes=[
            pltpu.VMEM((keys_count, inner), BF16),
            pltpu.VMEM((keys_count, inner), BF16),
            pltpu.VMEM((keys_count, LANES), BF16),
            pltpu.VMEM((tok_rows, LANES), BF16),
            pltpu.VMEM((inner, tok_rows), BF16),
            pltpu.VMEM(w_out.shape, BF16),
            *(pltpu.VMEM(o.shape, o.dtype) for o in window_shapes[:2]),
            pltpu.SemaphoreType.DMA((3,)),
        ],
        compiler_params=params(48000),
        cost_estimate=cost(4e9, 4e6),
        name="far",
    )(q, gates, mixed, w_out, *columns)


def solution(mesh):
    torus = Mesh(mesh.devices.reshape(mesh.shape["rep"], 4, 16, 2), REP_SEQ)

    return jax.shard_map(
        shards,
        mesh=torus,
        in_specs=(P(REP_SEQ, None), P(), P(), P(), P(), P(), P("rep")),
        out_specs=P(REP_SEQ, None),
        check_vma=False,
    )
```

```python
import functools

import jax
import jax.numpy as jnp
from jax import lax
from jax.experimental import pallas as pl
from jax.experimental.pallas import tpu as pltpu
from jax.sharding import Mesh
from jax.sharding import PartitionSpec as P

WINDOW = 128
REACH = 3
AX_X, AX_Z, AX_C = "seq_0", "seq_1", "seq_2"
SEQ = (AX_X, AX_Z, AX_C)
REP_SEQ = ("rep", AX_X, AX_Z, AX_C)
LANES = 128
NEG = -1e30
F32, BF16, I32 = jnp.float32, jnp.bfloat16, jnp.int32
NT = (((1,), (1,)), ((), ()))
TN = (((0,), (0,)), ((), ()))


def dot(a, b):
    return jnp.dot(a, b, preferred_element_type=F32)


def dot_nt(a, b):
    return lax.dot_general(a, b, NT, preferred_element_type=F32)


def iota(shape, dim):
    return lax.broadcasted_iota(I32, shape, dim)


def one_hot(condition):
    return jnp.where(condition, 1.0, 0.0).astype(BF16)


def half_lanes(rows):
    return iota((rows, LANES), 1) < LANES // 2


def token_classes(tok_rows, med_len):
    row, lane = iota((tok_rows, LANES), 0), iota((tok_rows, LANES), 1)
    wanted = 2 * (row // med_len) + jnp.where(row % med_len == med_len - 1, 1, 0)
    return one_hot(lane % (LANES // 2) == wanted)


def project_kernel(
    tok_hbm, w_hbm, cm_hbm, cc_hbm, kv_hbm, edge_ref, med_ref, pay_ref,
    tok_ref, w_buf, cm_ref, cc_ref, kv_ref, c_buf, sems, in_sems, out_sems,
):
    tok_rows = tok_ref.shape[0]
    _, _, med_len = cm_ref.shape
    coarse_len = cc_ref.shape[2]
    inner = kv_hbm.shape[1] // 2
    steps, _, width = kv_ref.shape
    fetches = [
        pltpu.make_async_copy(src, dst, in_sems.at[n])
        for n, (src, dst) in enumerate(((cm_hbm, cm_ref), (cc_hbm, cc_ref), (tok_hbm, tok_ref)))
    ]
    for fetch in fetches:
        fetch.start()
    copies = []
    chunk = w_buf.shape[0] // steps
    for g in range(steps):
        part = pl.ds(g * chunk, chunk)
        copies.append(
            pltpu.make_async_copy(w_hbm.at[part, pl.ds(inner, 2 * inner)], w_buf.at[part], sems.at[g])
        )
        copies[-1].start()
    med_blocks = tok_rows // med_len
    coarse_blocks = tok_rows // coarse_len
    per = width // 64
    tile_up = one_hot(iota((med_len, tok_rows), 1) % med_len == iota((med_len, tok_rows), 0))
    own_block = iota((per * med_blocks, tok_rows), 0) % med_blocks == (
        iota((per * med_blocks, tok_rows), 1) // med_len
    )
    own_coarse = iota((8, tok_rows), 0) == iota((8, tok_rows), 1) // coarse_len
    count = c_buf.shape[0]
    total = pay_ref.shape[0]
    repeat = one_hot(iota((total, count), 0) % count == iota((total, count), 1))
    fetches[0].wait()
    fetches[1].wait()
    mixes = []
    for g in range(steps):
        side, first = (2 * g) // steps, (g % (steps // 2)) * per
        med_rows, coarse_rows = [], []
        for i in range(per):
            med_w = cm_ref[first + i].astype(F32)[side : side + 1, :]
            med_rows.append(jnp.broadcast_to(med_w, (med_blocks, med_len)))
            coarse_w = cc_ref[first + i].astype(F32)[side : side + 1, :]
            coarse_w = jnp.concatenate([coarse_w] * coarse_blocks, axis=1)
            coarse_rows.append(jnp.where(own_coarse, jnp.broadcast_to(coarse_w, (8, tok_rows)), 0.0))
        med_mix = dot(jnp.concatenate(med_rows, 0).astype(BF16), tile_up)
        med_mix = jnp.where(own_block, med_mix, 0.0)
        mixes.append(jnp.concatenate([med_mix] + coarse_rows, 0).astype(BF16))
    fetches[2].wait()
    stores = []
    for copy in copies:
        copy.wait()
    all_rows = dot(tok_ref[...], w_buf[...]).astype(BF16)
    for g in range(steps):
        rows = all_rows[:, g * width : (g + 1) * width]
        kv_ref[g] = rows
        stores.append(
            pltpu.make_async_copy(kv_ref.at[g], kv_hbm.at[:, pl.ds(g * width, width)], out_sems.at[g])
        )
        stores[-1].start()
        packed = dot(mixes[g], rows)
        med_head = iota((med_blocks, width), 1) // 64
        coarse_head = iota((8, width), 1) // 64
        med = jnp.zeros((med_blocks, width), F32)
        coarse = jnp.zeros((8, width), F32)
        for i in range(per):
            med = jnp.where(med_head == i, packed[i * med_blocks : (i + 1) * med_blocks], med)
            at = per * med_blocks + 8 * i
            coarse = jnp.where(coarse_head == i, packed[at : at + 8], coarse)
        med_ref[:, g * width : (g + 1) * width] = med.astype(BF16)
        edge_ref[WINDOW:, g * width : (g + 1) * width] = med.astype(BF16)
        edge_ref[:WINDOW, g * width : (g + 1) * width] = rows[tok_rows - WINDOW :]
        for i in range(width // LANES):
            tile = g * (width // LANES) + i
            c_buf[tile * coarse_blocks : (tile + 1) * coarse_blocks, :] = coarse[
                :coarse_blocks, i * LANES : (i + 1) * LANES
            ]
    pay_ref[...] = dot(repeat, c_buf[...].astype(BF16)).astype(BF16)
    for store in stores:
        store.wait()


def values_up(tile, odd):
    eye = one_hot(iota((LANES, LANES), 0) == iota((LANES, LANES), 1))
    turned = dot_nt(eye, tile).astype(BF16)
    half = LANES // 2
    ones = jnp.ones((16, tile.shape[0]), BF16)
    return jnp.concatenate([turned[half * odd : half * (odd + 1)], ones], 0)


def device_position():
    return (lax.axis_index(AX_X) * lax.axis_size(AX_Z) + lax.axis_index(AX_Z)) * lax.axis_size(
        AX_C
    ) + lax.axis_index(AX_C)


def window_scores(keys, q_tile, odd, first_bias=None):
    below = iota((WINDOW, WINDOW), 0) <= iota((WINDOW, WINDOW), 1)
    mine = half_lanes(keys.shape[0]) if odd == 0 else ~half_lanes(keys.shape[0])
    k_ext = jnp.where(mine, keys, jnp.zeros_like(keys))
    merged = []
    for c in range(q_tile.shape[0] // WINDOW):
        s = dot_nt(k_ext[c * WINDOW : (c + 2) * WINDOW], q_tile[c * WINDOW : (c + 1) * WINDOW])
        left, right = s[:WINDOW], s[WINDOW:]
        if first_bias is not None:
            left = left + first_bias
        merged.append(jnp.where(below, right, left))
    return jnp.concatenate(merged, 1)


def window_values(scores, v_up, gate):
    below = iota((WINDOW, WINDOW), 0) <= iota((WINDOW, WINDOW), 1)
    half = LANES // 2
    terms = jnp.exp(scores - jnp.max(scores, axis=0, keepdims=True)).astype(BF16)
    outs = []
    for c in range(scores.shape[1] // WINDOW):
        part = terms[:, c * WINDOW : (c + 1) * WINDOW]
        zero = jnp.zeros_like(part)
        both = jnp.concatenate([jnp.where(below, zero, part), jnp.where(below, part, zero)], 0)
        outs.append(dot(v_up[:, c * WINDOW : (c + 2) * WINDOW], both))
    out = jnp.concatenate(outs, 1)
    return out[:half] * (gate / out[half : half + 1])


def window_kernel(early, tok_hbm, w_hbm, wg_ref, kv_hbm, *refs):
    (
        q_hbm, gate_hbm, mix_hbm,
        tok_ref, kv_ref, w_buf, q_ref, gate_ref, mix_ref, sems, in_sems, out_sems,
    ) = refs[-12:]
    low = lax.axis_index(AX_Z) < lax.axis_size(AX_Z) // 2

    @pl.when(low if early else jnp.logical_not(low))
    def _():
        inner = kv_ref.shape[1] // 2
        steps = sems.shape[0]
        chunk = w_buf.shape[0] // steps
        heads = gate_ref.shape[0] // 3
        half = LANES // 2
        fetch = pltpu.make_async_copy(tok_hbm, tok_ref, in_sems.at[0])
        fetch.start()
        copies = []
        for g in range(steps):
            copies.append(
                pltpu.make_async_copy(
                    w_hbm.at[pl.ds(g * chunk, chunk), pl.ds(0, inner)],
                    w_buf.at[pl.ds(g * chunk, chunk)],
                    sems.at[g],
                )
            )
            copies[-1].start()
        fetch_kv = pltpu.make_async_copy(kv_hbm, kv_ref, in_sems.at[1])
        fetch_kv.start()
        fetch.wait()
        gate_ref[...] = 1.0 / (1.0 + jnp.exp(-dot_nt(wg_ref[...], tok_ref[...])))
        for copy in copies:
            copy.wait()
        rows = dot(tok_ref[...], w_buf[...]).astype(BF16).astype(F32)
        q_ref[...] = (rows * (half**-0.5)).astype(BF16)
        fetch_kv.wait()

        @pl.loop(0, heads // 2)
        def _(pair):
            at = pl.multiple_of(pair * LANES, LANES)
            at_v = pl.multiple_of(inner + pair * LANES, LANES)
            q_tile = q_ref[WINDOW:, pl.ds(at, LANES)]
            keys = kv_ref[:, pl.ds(at, LANES)]
            values = kv_ref[:, pl.ds(at_v, LANES)]
            for odd in range(2):
                head = 2 * pair + odd
                scores = window_scores(keys, q_tile, odd)
                mix_ref[pl.ds(pl.multiple_of(head * half, half), half), :] = window_values(
                    scores, values_up(values, odd), gate_ref[pl.ds(head, 1), :][:, WINDOW:]
                )

        stores = [
            pltpu.make_async_copy(src, dst, out_sems.at[n])
            for n, (src, dst) in enumerate(((q_ref, q_hbm), (gate_ref, gate_hbm), (mix_ref, mix_hbm)))
        ]
        for store in stores:
            store.start()
        for store in stores:
            store.wait()


def medium_kernel(
    q_hbm, gate_hbm, old_hbm, kv_hbm, far3_ref, far2_ref, edge_ref, med_ref, gid_ref, mix_ref,
    q_ref, gate_ref, old_ref, kv_ref, bias_buf, hot_buf, sems,
):
    tok_rows, inner = q_ref.shape
    heads = gate_ref.shape[0] // 3
    med_blocks = med_ref.shape[0]
    near = (REACH + 1) * med_blocks
    half = LANES // 2
    moves = ((q_hbm, q_ref), (gate_hbm, gate_ref), (kv_hbm.at[pl.ds(0, WINDOW)], kv_ref), (old_hbm, old_ref))
    fetches = [pltpu.make_async_copy(src, dst, sems.at[n]) for n, (src, dst) in enumerate(moves)]
    for fetch in fetches:
        fetch.start()
    position = device_position()
    hot_buf[...] = token_classes(tok_rows, tok_rows // med_blocks)

    first = (position - REACH) * med_blocks
    padded = first + near
    row = padded // LANES - 1
    offset = padded % LANES
    low = gid_ref[pl.ds(jnp.maximum(row, 0), 1), :]
    high = gid_ref[pl.ds(jnp.minimum(row + 1, gid_ref.shape[0] - 1), 1), :]
    lane = iota((1, LANES), 1)
    both = jnp.where(lane >= offset, low, high)
    near_groups = pltpu.roll(jnp.broadcast_to(both, (8, LANES)), (LANES - offset) % LANES, 1)[:1]
    near_groups = jnp.where(lane + first >= 0, near_groups, -1).astype(F32)
    spread = jnp.broadcast_to(near_groups, (near, LANES)).astype(BF16)
    i0, i1 = iota((near, LANES), 0), iota((near, LANES), 1)
    key_group = dot_nt(one_hot(i0 == i1), spread)
    own = (i1 % half) // 2 + REACH * med_blocks
    token_group = dot(spread, one_hot(i0 == own))
    visible = (key_group == token_group) & ((i0 < own) | ((i0 == own) & (i1 % 2 == 1)))
    bias_buf[...] = jnp.where(visible, 0.0, NEG).astype(BF16)
    first_bias = jnp.where(position == 0, NEG, 0.0)
    for fetch in fetches:
        fetch.wait()

    @pl.loop(0, heads // 2, unroll=heads // 2)
    def _(pair):
        at = pl.multiple_of(pair * LANES, LANES)
        at_v = pl.multiple_of(inner + pair * LANES, LANES)
        q_tile = q_ref[:, pl.ds(at, LANES)]
        keys = jnp.concatenate([edge_ref[:WINDOW, pl.ds(at, LANES)], kv_ref[:, pl.ds(at, LANES)]], 0)
        values = jnp.concatenate(
            [edge_ref[:WINDOW, pl.ds(at_v, LANES)], kv_ref[:, pl.ds(at_v, LANES)]], 0
        )
        blocks = (far3_ref, far2_ref, edge_ref.at[pl.ds(WINDOW, med_blocks)], med_ref)
        med_k = jnp.concatenate([b[:, pl.ds(at, LANES)] for b in blocks], 0)
        med_v = jnp.concatenate([b[:, pl.ds(at_v, LANES)] for b in blocks], 0)
        both = dot_nt(pair_keys(med_k, bias_buf[...]), jnp.concatenate([q_tile, hot_buf[...]], 1))
        mine = half_lanes(2 * WINDOW)
        none = jnp.zeros_like(keys)
        rim_keys = jnp.concatenate([jnp.where(mine, keys, none), jnp.where(mine, none, keys)], 0)
        rims = dot_nt(rim_keys, q_tile[:WINDOW])
        below = iota((WINDOW, WINDOW), 0) <= iota((WINDOW, WINDOW), 1)
        for odd in range(2):
            head = 2 * pair + odd
            scores = both[odd * near : (odd + 1) * near]
            peak = jnp.maximum(jnp.max(scores, axis=0, keepdims=True), 0.0)
            terms = jnp.exp(scores - peak).astype(BF16)
            out = dot(values_up(med_v, odd), terms)
            factor = gate_ref[pl.ds(heads + head, 1), :] / (jnp.exp(-peak) + out[half : half + 1])
            at_rim = 2 * odd * WINDOW
            left, right = rims[at_rim : at_rim + WINDOW], rims[at_rim + WINDOW : at_rim + 2 * WINDOW]
            rim = window_values(
                jnp.where(below, right, left + first_bias),
                values_up(values, odd),
                gate_ref[pl.ds(head, 1), :][:, :WINDOW],
            )
            rows = pl.ds(pl.multiple_of(head * half, half), half)
            mix_ref[rows, :] = jnp.concatenate([rim, old_ref[rows, :]], 1) + out[:half] * factor


def pair_keys(keys, bias):
    mine = half_lanes(keys.shape[0])
    none = jnp.zeros_like(keys)
    bias = jnp.where(mine, bias, none)
    even = jnp.concatenate([jnp.where(mine, keys, none), bias], 1)
    return jnp.concatenate([even, jnp.concatenate([jnp.where(mine, none, keys), bias], 1)], 0)


def far_kernel(
    q_hbm, gate_hbm, mix_ref, w_hbm, *refs
):
    pieces, scratch = refs[:-10], refs[-10:]
    out_ref, keys_buf, values_buf, bias_buf, hot_buf, mixed_buf, w_ref, q_ref, gate_ref, sems = scratch
    moves = ((q_hbm, q_ref), (gate_hbm, gate_ref), (w_hbm, w_ref))
    fetches = [pltpu.make_async_copy(src, dst, sems.at[n]) for n, (src, dst) in enumerate(moves)]
    for fetch in fetches:
        fetch.start()
    tok_rows, inner = q_ref.shape
    heads = gate_ref.shape[0] // 3
    half = LANES // 2
    tiles = inner // LANES
    total = pieces[0].shape[0]
    zs = lax.axis_size(AX_Z)
    count = total // zs
    each = total // (2 * tiles)
    per = each // zs
    pos_x, pos_z, pos_c = lax.axis_index(AX_X), lax.axis_index(AX_Z), lax.axis_index(AX_C)
    xs, cs = lax.axis_size(AX_X), lax.axis_size(AX_C)
    hot_buf[...] = token_classes(tok_rows, 16)

    r0, r1 = iota((total, total), 0), iota((total, total), 1)
    source = ((r0 % each) // per) * count + (r0 // each) * per + r0 % per
    turn = one_hot(source == r1)
    sorted_rows = dot(turn, jnp.concatenate([p[...] for p in pieces], 1)).astype(BF16)
    lane = iota((each, LANES), 1) % half
    row = iota((each, LANES), 0)
    position = (pos_x * zs + pos_z) * cs + pos_c
    seen = per * position + jnp.where(lane >= half // per - 1, 1, 0) + jnp.where(lane == half - 1, 1, 0)
    for n in range(len(pieces)):
        for t in range(tiles):
            block = sorted_rows[t * each : (t + 1) * each, n * LANES : (n + 1) * LANES]
            keys_buf[n * each : (n + 1) * each, t * LANES : (t + 1) * LANES] = block
            block = sorted_rows[(tiles + t) * each : (tiles + t + 1) * each, n * LANES : (n + 1) * LANES]
            values_buf[n * each : (n + 1) * each, t * LANES : (t + 1) * LANES] = block
        from_x = lax.rem(pos_x + xs - n % xs, xs)
        from_c = lax.rem(pos_c + n // xs, cs)
        index = ((from_x * zs + row // per) * cs + from_c) * per + row % per
        bias_buf[n * each : (n + 1) * each, :] = jnp.where(index < seen, 0.0, NEG).astype(BF16)

    keys_count = keys_buf.shape[0]
    fetches[0].wait()
    fetches[1].wait()

    @pl.loop(0, tiles, unroll=tiles)
    def _(pair):
        at = pl.multiple_of(pair * LANES, LANES)
        q_ext = jnp.concatenate([q_ref[:, pl.ds(at, LANES)], hot_buf[...]], 1)
        values = values_buf[:, pl.ds(at, LANES)]
        both = dot_nt(pair_keys(keys_buf[:, pl.ds(at, LANES)], bias_buf[...]), q_ext)
        for odd in range(2):
            head = 2 * pair + odd
            scores = both[odd * keys_count : (odd + 1) * keys_count]
            peak = jnp.maximum(jnp.max(scores, axis=0, keepdims=True), 0.0)
            terms = jnp.exp(scores - peak).astype(BF16)
            out = dot(values_up(values, odd), terms)
            factor = gate_ref[pl.ds(2 * heads + head, 1), :] / (jnp.exp(-peak) + out[half : half + 1])
            rows = pl.ds(pl.multiple_of(head * half, half), half)
            mixed_buf[rows, :] = (mix_ref[rows, :] + out[:half] * factor).astype(BF16)

    fetches[2].wait()
    out_ref[...] = lax.dot_general(
        mixed_buf[...], w_ref[...], TN, preferred_element_type=F32
    ).astype(BF16)


def shifted(block, axis, distance):
    size = lax.axis_size(axis)
    return lax.ppermute(block, axis, [(i - distance, i) for i in range(distance, size)])


def turned(block, axis, distance):
    size = lax.axis_size(axis)
    return lax.ppermute(block, axis, [(i, (i + distance) % size) for i in range(size)])


VMEM = pl.BlockSpec(memory_space=pltpu.VMEM)
HBM = pl.BlockSpec(memory_space=pltpu.HBM)


def params(kib):
    return pltpu.CompilerParams(vmem_limit_bytes=kib << 10)


def cost(flops, moved):
    return pl.CostEstimate(flops=int(flops), bytes_accessed=int(moved), transcendentals=0)


def shards(tokens, w_qkv, w_gate, w_out, cmp_med, cmp_coarse, group_id):
    tok_rows, depth = tokens.shape
    heads, med_len, coarse_len = cmp_med.shape[1], cmp_med.shape[2], cmp_coarse.shape[2]
    inner = w_out.shape[0]
    width = 256
    med_blocks = tok_rows // med_len
    coarse_blocks = tok_rows // coarse_len
    zs = lax.axis_size(AX_Z)
    count = coarse_blocks * 2 * inner // LANES
    kv_steps = 2 * inner // width
    cmp_med, cmp_coarse = cmp_med.transpose(1, 0, 2), cmp_coarse.transpose(1, 0, 2)
    kv, edge, med, payload = pl.pallas_call(
        project_kernel,
        out_shape=(
            jax.ShapeDtypeStruct((tok_rows, 2 * inner), BF16),
            jax.ShapeDtypeStruct((WINDOW + med_blocks, 2 * inner), BF16),
            jax.ShapeDtypeStruct((med_blocks, 2 * inner), BF16),
            jax.ShapeDtypeStruct((zs * count, LANES), BF16),
        ),
        in_specs=[HBM] * 4,
        out_specs=(HBM, VMEM, VMEM, VMEM),
        scratch_shapes=[
            pltpu.VMEM(tokens.shape, BF16),
            pltpu.VMEM((depth, 2 * inner), BF16),
            pltpu.VMEM(cmp_med.shape, BF16),
            pltpu.VMEM(cmp_coarse.shape, BF16),
            pltpu.VMEM((kv_steps, tok_rows, width), BF16),
            pltpu.VMEM((count, LANES), F32),
            pltpu.SemaphoreType.DMA((kv_steps,)),
            pltpu.SemaphoreType.DMA((3,)),
            pltpu.SemaphoreType.DMA((kv_steps,)),
        ],
        compiler_params=params(58000),
        cost_estimate=cost(4e9, 4e6),
        name="project",
    )(tokens, w_qkv, cmp_med, cmp_coarse)

    q_steps = inner // width
    window_shapes = (
        jax.ShapeDtypeStruct((tok_rows, inner), BF16),
        jax.ShapeDtypeStruct((3 * heads, tok_rows), F32),
        jax.ShapeDtypeStruct((inner, tok_rows - WINDOW), F32),
    )

    def window(early, *given):
        return pl.pallas_call(
            functools.partial(window_kernel, early),
            out_shape=window_shapes,
            in_specs=[HBM, HBM, VMEM, HBM] + [HBM] * len(given),
            out_specs=(HBM, HBM, HBM),
            input_output_aliases={4 + n: n for n in range(len(given))},
            scratch_shapes=[
                pltpu.VMEM(tokens.shape, BF16),
                pltpu.VMEM((tok_rows, 2 * inner), BF16),
                pltpu.VMEM((depth, inner), BF16),
                *(pltpu.VMEM(o.shape, o.dtype) for o in window_shapes),
                pltpu.SemaphoreType.DMA((q_steps,)),
                pltpu.SemaphoreType.DMA((2,)),
                pltpu.SemaphoreType.DMA((3,)),
            ],
            compiler_params=params(54000),
            cost_estimate=cost(8e9, 8e6),
            name="window",
        )(tokens, w_qkv, w_gate.T, kv, *given)

    parts = window(True)
    column = lax.all_to_all(payload, AX_Z, 0, 0, tiled=True)
    edge1 = shifted(edge, SEQ, 1)
    far2, far3 = shifted(med, SEQ, 2), shifted(med, SEQ, 3)
    q, gates, mixed = window(False, *parts)
    columns = [column] + [turned(column, AX_X, k) for k in range(1, lax.axis_size(AX_X))]
    mixed = pl.pallas_call(
        medium_kernel,
        out_shape=jax.ShapeDtypeStruct((inner, tok_rows), F32),
        in_specs=[HBM] * 4 + [VMEM] * 5,
        out_specs=VMEM,
        scratch_shapes=[
            *(pltpu.VMEM(o.shape, o.dtype) for o in window_shapes),
            pltpu.VMEM((WINDOW, 2 * inner), BF16),
            pltpu.VMEM(((REACH + 1) * med_blocks, LANES), BF16),
            pltpu.VMEM((tok_rows, LANES), BF16),
            pltpu.SemaphoreType.DMA((4,)),
        ],
        compiler_params=params(50000),
        cost_estimate=cost(4e9, 4e6),
        name="medium",
    )(q, gates, mixed, kv, far3, far2, edge1, med, group_id.reshape(-1, LANES))
    columns += [turned(c, AX_C, 1) for c in columns]
    keys_count = coarse_blocks * lax.axis_size(SEQ)
    return pl.pallas_call(
        far_kernel,
        out_shape=jax.ShapeDtypeStruct((tok_rows, inner), BF16),
        in_specs=[HBM, HBM, VMEM, HBM] + [VMEM] * len(columns),
        out_specs=VMEM,
        scratch_shapes=[
            pltpu.VMEM((keys_count, inner), BF16),
            pltpu.VMEM((keys_count, inner), BF16),
            pltpu.VMEM((keys_count, LANES), BF16),
            pltpu.VMEM((tok_rows, LANES), BF16),
            pltpu.VMEM((inner, tok_rows), BF16),
            pltpu.VMEM(w_out.shape, BF16),
            *(pltpu.VMEM(o.shape, o.dtype) for o in window_shapes[:2]),
            pltpu.SemaphoreType.DMA((3,)),
        ],
        compiler_params=params(48000),
        cost_estimate=cost(4e9, 4e6),
        name="far",
    )(q, gates, mixed, w_out, *columns)


def solution(mesh):
    torus = Mesh(mesh.devices.reshape(mesh.shape["rep"], 4, 16, 2), REP_SEQ)

    return jax.shard_map(
        shards,
        mesh=torus,
        in_specs=(P(REP_SEQ, None), P(), P(), P(), P(), P(), P("rep")),
        out_specs=P(REP_SEQ, None),
        check_vma=False,
    )
```
